8 devices in a mesh: dp: 2 (over z, y), row: 2 (over x), fsdp: 2 (over core).
Axes of the slice: x: 2, y: 2, z: 1, core: 2. Of those that a mesh axis runs over, the one named last changes fastest.
Arguments:
- x_in: bfloat16 [32768, 512], P(('dp', 'row', 'fsdp'))
- dy_out: bfloat16 [32768, 512], P(('dp', 'row', 'fsdp'))
- w_gate: bfloat16 [512, 1376], P(None, ('row', 'fsdp'))
- w_up: bfloat16 [512, 1376], P(None, ('row', 'fsdp'))
- w_down: bfloat16 [1376, 512], P(('row', 'fsdp'))
- g_next: float32 [8, 3, 512, 1376], P(('dp', 'row', 'fsdp'))
Outputs:
- output 1: bfloat16 [32768, 512], P(('dp', 'row', 'fsdp'))
- output 2: float32 [3, 512, 1376], P(None, None, ('row', 'fsdp'))
- output 3: float32 [8, 3, 512, 1376], P(('dp', 'row', 'fsdp'))
All inputs are finite; a program needn't handle non-finite values.
Results may differ from the reference program's by a relative error of at most 0.0108858.
Values are sent between devices in bfloat16 or wider.
A program may use at most 1 GiB of HBM per device.

```python
import jax
import jax.numpy as jnp
from jax import lax
import math

MODEL_DIM = 512
HIDDEN_DIM = 1376
TOKENS_DEV = 4096
DEVICES = 8


def setup_inputs(seed: int = 0) -> dict:
    rand_keys = jax.random.split(jax.random.key(seed), 6)
    act_shape = (DEVICES * TOKENS_DEV, MODEL_DIM)
    in_scale = 1.0 / math.sqrt(MODEL_DIM)
    hid_scale = 1.0 / math.sqrt(HIDDEN_DIM)
    x_in = jax.random.normal(rand_keys[0], act_shape, jnp.float32).astype(jnp.bfloat16)
    dy_out = jax.random.normal(rand_keys[1], act_shape, jnp.float32).astype(jnp.bfloat16)
    w_gate = (jax.random.normal(rand_keys[2], (MODEL_DIM, HIDDEN_DIM), jnp.float32) * in_scale).astype(jnp.bfloat16)
    w_up = (jax.random.normal(rand_keys[3], (MODEL_DIM, HIDDEN_DIM), jnp.float32) * in_scale).astype(jnp.bfloat16)
    w_down = (jax.random.normal(rand_keys[4], (HIDDEN_DIM, MODEL_DIM), jnp.float32) * hid_scale).astype(jnp.bfloat16)
    g_next = jax.random.normal(rand_keys[5], (DEVICES, 3, MODEL_DIM, HIDDEN_DIM), jnp.float32)
    return {"x_in": x_in, "dy_out": dy_out, "w_gate": w_gate, "w_up": w_up, "w_down": w_down, "g_next": g_next}


def local_backward(x_blk, dy_blk, w_gate, w_up, w_down):
    a_pre = jnp.dot(x_blk, w_gate, preferred_element_type=jnp.float32)
    b_pre = jnp.dot(x_blk, w_up, preferred_element_type=jnp.float32)
    sig_a = jax.nn.sigmoid(a_pre)
    silu_a = a_pre * sig_a
    h_act = (silu_a * b_pre).astype(jnp.bfloat16)
    dh_full = jnp.dot(dy_blk, w_down.T, preferred_element_type=jnp.float32)
    da_bf = (dh_full * b_pre * sig_a * (1.0 + a_pre * (1.0 - sig_a))).astype(jnp.bfloat16)
    db_bf = (dh_full * silu_a).astype(jnp.bfloat16)
    dx_acc = jnp.dot(da_bf, w_gate.T, preferred_element_type=jnp.float32) + jnp.dot(db_bf, w_up.T, preferred_element_type=jnp.float32)
    grad_gate = jnp.dot(x_blk.T, da_bf, preferred_element_type=jnp.float32)
    grad_up = jnp.dot(x_blk.T, db_bf, preferred_element_type=jnp.float32)
    grad_down = jnp.dot(dy_blk.T, h_act, preferred_element_type=jnp.float32)
    return dx_acc.astype(jnp.bfloat16), jnp.stack([grad_gate, grad_up, grad_down])


def reference(x_in, dy_out, w_gate, w_up, w_down, g_next):
    x_blocks = x_in.reshape(DEVICES, TOKENS_DEV, MODEL_DIM)
    dy_blocks = dy_out.reshape(DEVICES, TOKENS_DEV, MODEL_DIM)

    def per_device(block_pair):
        return local_backward(block_pair[0], block_pair[1], w_gate, w_up, w_down)

    dx_blocks, dw_local = lax.map(per_device, (x_blocks, dy_blocks))
    dx_in = dx_blocks.reshape(DEVICES * TOKENS_DEV, MODEL_DIM)
    dw_next = jnp.sum(g_next.astype(jnp.bfloat16).astype(jnp.float32), axis=0)
    return (dx_in, dw_next, dw_local)
```

```python
import functools

import jax
import jax.numpy as jnp
from jax import lax
from jax.experimental import pallas as pl
from jax.experimental.pallas import tpu as pltpu
from jax.sharding import PartitionSpec as P

GROUP_AXES = ("row", "fsdp")
ALL_AXES = ("dp", "row", "fsdp")
MESH = pl.DeviceIdType.MESH
BF, F32 = jnp.bfloat16, jnp.float32

T, D, H = 4096, 512, 1376
HS = H // 4
HSP = 384
HQ = 2 * HSP
TB = 1024
NBLK = T // TB
NCH, CW = 6, 256
NWP, WW = 6, 128

NN = (((1,), (0,)), ((), ()))
NT = (((1,), (1,)), ((), ()))
TN = (((0,), (0,)), ((), ()))


def dot(a, b, dims):
    return lax.dot_general(a, b, dims, preferred_element_type=F32)


def gate_grads(a, b, dh):
    sig = 0.5 * jnp.tanh(0.5 * a) + 0.5
    silu = a * sig
    h = (silu * b).astype(BF)
    da = (dh * b * sig * (1.0 + a * (1.0 - sig))).astype(BF)
    db = (dh * silu).astype(BF)
    return h, da, db


def step_kernel(nb1, x_hbm, dy_hbm, w1_hbm, w3_hbm, w2_hbm, g_hbm, dx_hbm, dwt_hbm, gn_hbm,
                x, dy, wall, dxa, dxs, dab, dw, gst, pk, prec, xrec, yrec, gn,
                x_sem, dy_sem, ws_sem, g_sem, dx_sem, dw_sem, gn_sem,
                a1s, a1r, a2s, a2r, a3s, a3r, a4s, a4r, ps, pr, xs_, xr_, ys_, yr_):
    dp, row, f = (lax.axis_index(n) for n in ALL_AXES)
    partner, xn, yn = {"fsdp": 1 - f}, {"row": 1 - row}, {"dp": 1 - dp}
    mine = pl.ds(pl.multiple_of(f * HSP, HSP), HS)

    def xload(i):
        rows = pl.ds(pl.multiple_of(i * TB, TB), TB)
        return (pltpu.make_async_copy(x_hbm.at[rows], x.at[rows], x_sem.at[i]),
                pltpu.make_async_copy(dy_hbm.at[rows], dy.at[rows], dy_sem.at[i]))

    def gload(c):
        return pltpu.make_async_copy(g_hbm.at[c // 2, :, :, pl.ds((c % 2) * CW, CW)], gst.at[c % 3], g_sem.at[c % 3])

    def remote(src, dst, s, r, dev):
        return pltpu.make_async_remote_copy(src_ref=src, dst_ref=dst, send_sem=s, recv_sem=r, device_id=dev, device_id_type=MESH)

    def wload(m):
        return pltpu.make_async_copy((w1_hbm, w3_hbm, w2_hbm)[m], wall.at[0, m, mine], ws_sem.at[m])

    def a1(m):
        ref = wall.at[0, m, mine]
        return remote(ref, ref, a1s.at[m], a1r.at[m], partner)

    def piece(p, j, half):
        return wall.at[p, j // 2, mine, pl.ds(pl.multiple_of(half * 256 + (j % 2) * WW, WW), WW)]

    def a2(j):
        return remote(piece(0, j, dp), piece(1, j, dp), a2s.at[j], a2r.at[j], xn)

    def a3(j):
        ref = piece(1, j, dp)
        return remote(ref, ref, a3s.at[j], a3r.at[j], yn)

    def a4(n, j, half):
        ref = piece(1, j, half)
        return remote(ref, ref, a4s.at[n, j], a4r.at[n, j], partner)

    def psend(c):
        return remote(pk.at[c, 1 - f], prec.at[c], ps.at[c], pr.at[c], partner)

    def xsend(c):
        return remote(pk.at[c, f, 1 - row], xrec.at[c], xs_.at[c], xr_.at[c], xn)

    def ysend(c):
        return remote(pk.at[c, f, row], yrec.at[c], ys_.at[c], yr_.at[c], yn)

    edge = HS // 16 * 16
    for p in range(2):
        for m in range(3):
            for k in range(2):
                wall[p, m, k * HSP + edge:(k + 1) * HSP, :] = jnp.zeros((HSP - edge, D), BF)
    for m in range(3):
        wload(m).start()
    for c in range(3):
        gload(c).start()
    barrier = pltpu.get_barrier_semaphore()
    for dev in (partner, xn, yn):
        pl.semaphore_signal(barrier, inc=1, device_id=dev, device_id_type=MESH)
    pl.semaphore_wait(barrier, 3)
    for m in range(3):
        wload(m).wait()
        a1(m).start()
        a2(2 * m).start()
        a2(2 * m + 1).start()
    for cp in xload(0):
        cp.start()
    for c in range(NCH):
        gload(c).wait()
        for s in range(4):
            pk[c, s % 2, s // 2] = gst[c % 3, s].astype(BF)
        if c + 3 < NCH:
            gload(c + 3).start()
        if c > 0:
            psend(c - 1).start()
    for i in range(1, NBLK):
        for cp in xload(i):
            cp.start()
    psend(NCH - 1).start()
    for m in range(3):
        a1(m).wait_recv()

    def add1(c):
        psend(c).wait_recv()
        for k in range(2):
            pk[c, f, k] = (pk[c, f, k].astype(F32) + prec[c, k].astype(F32)).astype(BF)

    def add2(c):
        xsend(c).wait_recv()
        pk[c, f, row] = (pk[c, f, row].astype(F32) + xrec[c].astype(F32)).astype(BF)

    def fin(c):
        ysend(c).wait_recv()
        total = pk[c, f, row].astype(F32) + yrec[c].astype(F32)
        gn[c // 2, :, pl.ds(pl.multiple_of((c % 2) * CW, CW), CW)] = total

    def w_first(j):
        a2(j).wait_recv()
        a3(j).start()
        a4(0, j, dp).start()

    def w_second(j):
        a3(j).wait_recv()
        a4(1, j, 1 - dp).start()

    plan = [
        (2, 1, NWP, w_first),
        (4, 1, NWP, w_second),
        (2, 1, NCH, lambda c: xsend(c).start()),
        (1, 1, NCH, add1),
        (9, 2, NCH, lambda c: ysend(c).start()),
        (8, 2, NCH, add2),
        (12, 2, NCH, fin),
    ]

    def comm(q, lo, hi, sub):
        for first, stride, count, action in plan:
            last = first + stride * (count - 1)
            points = [n for n in range(first, last + 1, stride) if lo <= n < hi and n % 3 == sub]
            if points:
                ok = (q >= first) & (q <= last)
                if stride > 1:
                    ok = ok & ((q - first) % stride == 0)
                c = jnp.clip((q - first) // stride, 0, count - 1)
                pl.when(ok)(functools.partial(action, c))

    def run(p, nblocks):
        lo, hi = p * 3 * NBLK, p * 3 * NBLK + 3 * nblocks

        def body(i, carry):
            q = lo + 3 * i
            rows = pl.ds(pl.multiple_of(i * TB, TB), TB)
            if p == 0:
                for cp in xload(i):
                    cp.wait()
            else:
                slot = i % 2

                @pl.when(i >= 2)
                def _():
                    dx_out(i - 2).wait()
            comm(q, lo, hi, 0)
            xb, dyb = x[rows, :], dy[rows, :]
            a = dot(xb, wall[p, 0], NT)
            b = dot(xb, wall[p, 1], NT)
            dh = dot(dyb, wall[p, 2], NT)
            h, da, db = gate_grads(a, b, dh)
            dab[0], dab[1], dab[2] = da, db, h
            comm(q + 1, lo, hi, 1)
            r = dot(dab[0], wall[p, 0], NN) + dot(dab[1], wall[p, 1], NN)
            if p == 0:
                dxa[rows, :] = r
            else:
                dxs[slot] = (dxa[rows, :] + r).astype(BF)
            comm(q + 2, lo, hi, 2)
            if p == 1:
                dx_out(i).start()

                @pl.when(i == 0)
                def _():
                    dw_out(0).wait()
            xb, dyb = x[rows, :], dy[rows, :]
            for k in range(3):
                for s in range(2):
                    part = dot(dab[k, :, s * HSP:s * HSP + HS], dyb if k == 2 else xb, TN)
                    dw[k, s] = jnp.where(i == 0, 0.0, dw[k, s]) + part
            return carry

        lax.fori_loop(0, nblocks, body, 0)

    def dx_out(i):
        rows = pl.ds(pl.multiple_of(i * TB, TB), TB)
        return pltpu.make_async_copy(dxs.at[i % 2], dx_hbm.at[rows], dx_sem.at[i % 2])

    def dw_out(p):
        return pltpu.make_async_copy(dw, dwt_hbm.at[:, pl.ds(2 * (row if p == 0 else 1 - row), 2)], dw_sem)

    run(0, NBLK)
    dw_out(0).start()
    for j in range(NWP):
        a4(0, j, dp).wait_recv()
        a4(1, j, 1 - dp).wait_recv()
    run(1, nb1)
    dw_out(1).start()

    gn_copy = pltpu.make_async_copy(gn, gn_hbm, gn_sem)
    gn_copy.start()
    for m in range(3):
        a1(m).wait_send()
    for j in range(NWP):
        a2(j).wait_send()
        a3(j).wait_send()
        a4(0, j, dp).wait_send()
        a4(1, j, 1 - dp).wait_send()
    for c in range(NCH):
        psend(c).wait_send()
        xsend(c).wait_send()
        ysend(c).wait_send()
    dx_out(nb1 - 2).wait()
    dx_out(nb1 - 1).wait()
    dw_out(1).wait()
    gn_copy.wait()


def fused_step(x, dy, w1, w3, w2, g):
    any_space = pl.BlockSpec(memory_space=pl.ANY)
    dma = pltpu.SemaphoreType.DMA
    scratch = [
        pltpu.VMEM((T, D), BF), pltpu.VMEM((T, D), BF), pltpu.VMEM((2, 3, HQ, D), BF),
        pltpu.VMEM((T, D), F32), pltpu.VMEM((2, TB, D), BF), pltpu.VMEM((3, TB, HQ), BF), pltpu.VMEM((3, 2, HS, D), F32),
        pltpu.VMEM((3, 4, HS, CW), F32), pltpu.VMEM((NCH, 2, 2, HS, CW), BF), pltpu.VMEM((NCH, 2, HS, CW), BF),
        pltpu.VMEM((NCH, HS, CW), BF), pltpu.VMEM((NCH, HS, CW), BF), pltpu.VMEM((3, HS, D), F32),
        dma((NBLK,)), dma((NBLK,)), dma((3,)), dma((3,)), dma((2,)), dma, dma,
        dma((3,)), dma((3,)), dma((NWP,)), dma((NWP,)), dma((NWP,)), dma((NWP,)), dma((2, NWP)), dma((2, NWP)),
        dma((NCH,)), dma((NCH,)), dma((NCH,)), dma((NCH,)), dma((NCH,)), dma((NCH,)),
    ]
    return pl.pallas_call(
        functools.partial(step_kernel, NBLK),
        out_shape=(jax.ShapeDtypeStruct((T, D), BF), jax.ShapeDtypeStruct((3, 4, HS, D), F32), jax.ShapeDtypeStruct((3, HS, D), F32)),
        in_specs=[any_space] * 6,
        out_specs=(any_space,) * 3,
        scratch_shapes=scratch,
        compiler_params=pltpu.CompilerParams(collective_id=0, has_side_effects=True, vmem_limit_bytes=67043328),
    )(x, dy, w1, w3, w2, g)


def solution(mesh):
    def per_device(x_blk, dy_blk, gate_shard, up_shard, down_shard, g_part):
        g_t = jnp.swapaxes(g_part[0], 1, 2).reshape(3, 4, HS, D)
        dx_blk, dwt, gnt = fused_step(x_blk, dy_blk, gate_shard.T, up_shard.T, down_shard, g_t)
        dw_local = jnp.swapaxes(dwt.reshape(3, H, D), 1, 2)
        return dx_blk, jnp.swapaxes(gnt, 1, 2), dw_local[None]

    return jax.shard_map(
        per_device,
        mesh=mesh,
        in_specs=(P(ALL_AXES, None), P(ALL_AXES, None), P(None, GROUP_AXES), P(None, GROUP_AXES), P(GROUP_AXES, None), P(ALL_AXES, None, None, None)),
        out_specs=(P(ALL_AXES, None), P(None, None, GROUP_AXES), P(ALL_AXES, None, None, None)),
        check_vma=False,
    )
```

```python
import functools

import jax
import jax.numpy as jnp
from jax import lax
from jax.experimental import pallas as pl
from jax.experimental.pallas import tpu as pltpu
from jax.sharding import PartitionSpec as P

GROUP_AXES = ("row", "fsdp")
ALL_AXES = ("dp", "row", "fsdp")
MESH = pl.DeviceIdType.MESH
BF, F32 = jnp.bfloat16, jnp.float32

T, D, H = 4096, 512, 1376
HS = H // 4
HSP = 384
HQ = 2 * HSP
TB = 1024
NBLK = T // TB
NCH, CW = 6, 256
NWP, WW = 6, 128
NT_COLS, GATE_ROWS = 256, 64
NB1 = 2

NN = (((1,), (0,)), ((), ()))
NT = (((1,), (1,)), ((), ()))
TN = (((0,), (0,)), ((), ()))


def dot(a, b, dims):
    return lax.dot_general(a, b, dims, preferred_element_type=F32)


def gate_grads(a, b, dh):
    sig = 0.5 * jnp.tanh(0.5 * a) + 0.5
    silu = a * sig
    h = (silu * b).astype(BF)
    da = (dh * b * sig * (1.0 + a * (1.0 - sig))).astype(BF)
    db = (dh * silu).astype(BF)
    return h, da, db


def block_rows(i):
    return pl.ds(i * TB if isinstance(i, int) else pl.multiple_of(i * TB, TB), TB)


def activations(xb, dyb, w, dab):
    for c in range(0, HQ, NT_COLS):
        cols = slice(c, c + NT_COLS)
        a = dot(xb, w[0, cols], NT)
        b = dot(xb, w[1, cols], NT)
        dh = dot(dyb, w[2, cols], NT)
        for r in range(0, TB, GATE_ROWS):
            rows = slice(r, r + GATE_ROWS)
            h, da, db = gate_grads(a[rows], b[rows], dh[rows])
            dab[0, rows, cols], dab[1, rows, cols], dab[2, rows, cols] = da, db, h


def input_grad(w, dab):
    return dot(dab[0], w[0], NN) + dot(dab[1], w[1], NN)


def weight_grad(k, xb, dyb, dab, dw, fresh):
    for s in range(2):
        part = dot(dab[k, :, s * HSP:s * HSP + HS], dyb if k == 2 else xb, TN)
        if fresh is True:
            dw[k, s] = part
        elif fresh is False:
            dw[k, s] = dw[k, s] + part
        else:
            dw[k, s] = jnp.where(fresh, 0.0, dw[k, s]) + part


def first_kernel(x_hbm, dy_hbm, w1_hbm, w3_hbm, w2_hbm, g_hbm,
                 dxr_hbm, dxa_hbm, dw0_hbm, dwa_hbm, w_hbm, gp_hbm, gy_hbm,
                 x, dy, wall, dxa, dxs, dab, dw, gst, pk, prec, xrec,
                 x_sem, dy_sem, ws_sem, g_sem, dx_sem, dxa_sem, dw0_sem, dwa_sem, w_sem, gp_sem,
                 a1s, a1r, a2s, a2r, a3s, a3r, a4s, a4r, ps, pr, xs_, xr_, ys_, yr_):
    dp, row, f = (lax.axis_index(n) for n in ALL_AXES)
    partner, xn, yn = {"fsdp": 1 - f}, {"row": 1 - row}, {"dp": 1 - dp}
    mine = pl.ds(pl.multiple_of(f * HSP, HSP), HS)

    def xload(i):
        rows = block_rows(i)
        return (pltpu.make_async_copy(x_hbm.at[rows], x.at[rows], x_sem.at[i]),
                pltpu.make_async_copy(dy_hbm.at[rows], dy.at[rows], dy_sem.at[i]))

    def gload(c):
        return pltpu.make_async_copy(g_hbm.at[c // 2, :, :, pl.ds((c % 2) * CW, CW)], gst.at[c % 3], g_sem.at[c % 3])

    def remote(src, dst, s, r, dev):
        return pltpu.make_async_remote_copy(src_ref=src, dst_ref=dst, send_sem=s, recv_sem=r, device_id=dev, device_id_type=MESH)

    def wload(m):
        return pltpu.make_async_copy((w1_hbm, w3_hbm, w2_hbm)[m], wall.at[0, m, mine], ws_sem.at[m])

    def a1(m):
        ref = wall.at[0, m, mine]
        return remote(ref, ref, a1s.at[m], a1r.at[m], partner)

    def piece(p, j, half):
        return wall.at[p, j // 2, mine, pl.ds(pl.multiple_of(half * 256 + (j % 2) * WW, WW), WW)]

    def a2(j):
        return remote(piece(0, j, dp), piece(1, j, dp), a2s.at[j], a2r.at[j], xn)

    def a3(j):
        ref = piece(1, j, dp)
        return remote(ref, ref, a3s.at[j], a3r.at[j], yn)

    def a4(n, j, half):
        ref = piece(1, j, half)
        return remote(ref, ref, a4s.at[n, j], a4r.at[n, j], partner)

    def psend(c):
        return remote(pk.at[c, 1 - f], prec.at[c], ps.at[c], pr.at[c], partner)

    def xsend(c):
        return remote(pk.at[c, f, 1 - row], xrec.at[c], xs_.at[c], xr_.at[c], xn)

    def ysend(c):
        return remote(pk.at[c, f, row], gy_hbm.at[c], ys_.at[c], yr_.at[c], yn)

    def gp_out(c):
        return pltpu.make_async_copy(pk.at[c, f, row], gp_hbm.at[c], gp_sem.at[c])

    def dx_out(i):
        return pltpu.make_async_copy(dxs.at[i % 2], dxr_hbm.at[block_rows(i)], dx_sem.at[i % 2])

    def dwa_out(k):
        return pltpu.make_async_copy(dw.at[k], dwa_hbm.at[k], dwa_sem.at[k])

    dw0_out = pltpu.make_async_copy(dw, dw0_hbm, dw0_sem)
    dxa_out = pltpu.make_async_copy(dxa.at[pl.ds(NB1 * TB, T - NB1 * TB)], dxa_hbm, dxa_sem)
    w_out = pltpu.make_async_copy(wall.at[1], w_hbm, w_sem)

    def convert(c):
        gload(c).wait()
        for s in range(4):
            pk[c, s % 2, s // 2] = gst[c % 3, s].astype(BF)

    edge = HS // 16 * 16
    for p in range(2):
        for m in range(3):
            for k in range(2):
                wall[p, m, k * HSP + edge:(k + 1) * HSP, :] = jnp.zeros((HSP - edge, D), BF)
    for m in range(3):
        wload(m).start()
    for c in range(2):
        gload(c).start()
    for cp in xload(0):
        cp.start()
    gload(2).start()
    barrier = pltpu.get_barrier_semaphore()
    for dev in (partner, xn, yn):
        pl.semaphore_signal(barrier, inc=1, device_id=dev, device_id_type=MESH)
    pl.semaphore_wait(barrier, 3)
    for m in range(3):
        wload(m).wait()
        a1(m).start()
        a2(2 * m).start()
        a2(2 * m + 1).start()
    for c in range(2):
        convert(c)
        gload(c + 3).start()
    for i in range(1, NBLK):
        for cp in xload(i):
            cp.start()
    for c in range(2):
        psend(c).start()
    for m in range(3):
        a1(m).wait_recv()

    def add1(c):
        psend(c).wait_recv()
        for k in range(2):
            pk[c, f, k] = (pk[c, f, k].astype(F32) + prec[c, k].astype(F32)).astype(BF)

    def add2(c):
        xsend(c).wait_recv()
        pk[c, f, row] = (pk[c, f, row].astype(F32) + xrec[c].astype(F32)).astype(BF)

    def w_first(j):
        a2(j).wait_recv()
        a3(j).start()
        a4(0, j, dp).start()

    def w_second(j):
        a3(j).wait_recv()
        a4(1, j, 1 - dp).start()

    plan = {
        1: ((0,), (), (2, 3, 4), (), ()),
        2: ((1, 2), (), (5,), (0, 1), ()),
        3: ((3,), (0,), (), (2, 3, 4), ()),
        4: ((4, 5), (1,), (), (5,), ()),
        5: ((), (2, 3), (), (), (0,)),
        6: ((), (4, 5), (), (), (1,)),
        7: ((), (), (), (), (2,)),
        8: ((), (), (), (), (3,)),
        10: ((), (), (), (), (4,)),
        11: ((), (), (), (), (5,)),
    }

    def actions(n):
        first, second, conv, chip, over_x = plan[n]
        for j in first:
            w_first(j)
        for j in second:
            w_second(j)
        for c in conv:
            convert(c)
            if c + 3 < NCH:
                gload(c + 3).start()
        for c in chip:
            add1(c)
        for c in over_x:
            add2(c)
        for c in conv:
            psend(c).start()
        for c in chip:
            xsend(c).start()
        for c in over_x:
            ysend(c).start()
            gp_out(c).start()

    def body(i, carry):
        rows = block_rows(i)
        for cp in xload(i):
            cp.wait()
        for blk in range(NBLK):
            if 2 * blk in plan:
                pl.when(i == blk)(functools.partial(actions, 2 * blk))
        activations(x[rows, :], dy[rows, :], wall.at[0], dab)
        for blk in range(NBLK):
            if 2 * blk + 1 in plan:
                pl.when(i == blk)(functools.partial(actions, 2 * blk + 1))
        dxa[rows, :] = input_grad(wall.at[0], dab)
        for k in range(3):
            weight_grad(k, x[rows, :], dy[rows, :], dab, dw, i == 0)
        return carry

    lax.fori_loop(0, NBLK, body, 0)
    dw0_out.start()
    dxa_out.start()
    for j in range(NWP):
        a4(0, j, dp).wait_recv()
        a4(1, j, 1 - dp).wait_recv()
    w_out.start()

    for i in range(NB1):
        rows = block_rows(i)
        n = 2 * (NBLK + i)
        if n in plan:
            actions(n)
        activations(x[rows, :], dy[rows, :], wall.at[1], dab)
        if n + 1 in plan:
            actions(n + 1)
        dxs[i % 2] = (dxa[rows, :] + input_grad(wall.at[1], dab)).astype(BF)
        if i == 0:
            dw0_out.wait()
        for k in range(3):
            weight_grad(k, x[rows, :], dy[rows, :], dab, dw, i == 0)
            if i == NB1 - 1:
                dwa_out(k).start()
        dx_out(i).start()

    for m in range(3):
        a1(m).wait_send()
    for j in range(NWP):
        a2(j).wait_send()
        a3(j).wait_send()
        a4(0, j, dp).wait_send()
        a4(1, j, 1 - dp).wait_send()
    for c in range(NCH):
        psend(c).wait_send()
        xsend(c).wait_send()
        ysend(c).wait_send()
        gp_out(c).wait()
    for i in range(NB1):
        dx_out(i).wait()
    dxa_out.wait()
    w_out.wait()
    for k in range(3):
        dwa_out(k).wait()
    for c in range(NCH):
        ysend(c).wait_recv()


def second_kernel(x_hbm, dy_hbm, dxr_hbm, dxa_hbm, dw0_hbm, dwa_hbm, w_hbm, gp_hbm, gy_hbm,
                  dx_hbm, dwt_hbm, gn_hbm,
                  x, dy, w, dxr, dxa, dxs, dab, dw, dw0, gp, gy, gn,
                  x_sem, dy_sem, w_sem, dxa_sem, in_sem, dx_sem, dw_sem, out_sem):
    row = lax.axis_index("row")
    nb = NBLK - NB1

    def xload(i):
        rows = block_rows(NB1 + i)
        return (pltpu.make_async_copy(x_hbm.at[rows], x.at[i], x_sem.at[i]),
                pltpu.make_async_copy(dy_hbm.at[rows], dy.at[i], dy_sem.at[i]),
                pltpu.make_async_copy(dxa_hbm.at[block_rows(i)], dxa.at[i], dxa_sem.at[i]))

    def dx_out(i):
        return pltpu.make_async_copy(dxs.at[i], dx_hbm.at[block_rows(NB1 + i)], dx_sem.at[i])

    def dw_out(k):
        return pltpu.make_async_copy(dw.at[k], dwt_hbm.at[k, pl.ds(2 * (1 - row), 2)], dw_sem.at[k])

    w_in = pltpu.make_async_copy(w_hbm, w, w_sem)
    dwa_in, gp_in, gy_in, dxr_in, dw0_in = (
        pltpu.make_async_copy(src, dst, in_sem.at[n])
        for n, (src, dst) in enumerate([(dwa_hbm, dw), (gp_hbm, gp), (gy_hbm, gy), (dxr_hbm, dxr), (dw0_hbm, dw0)]))
    dxr_out = pltpu.make_async_copy(dxr, dx_hbm.at[pl.ds(0, NB1 * TB)], out_sem.at[0])
    dw0_out = pltpu.make_async_copy(dw0, dwt_hbm.at[:, pl.ds(2 * row, 2)], out_sem.at[1])
    gn_out = pltpu.make_async_copy(gn, gn_hbm, out_sem.at[2])

    w_in.start()
    for cp in xload(0):
        cp.start()
    dwa_in.start()
    for i in range(1, nb):
        for cp in xload(i):
            cp.start()
    for cp in (gp_in, gy_in, dxr_in, dw0_in):
        cp.start()
    w_in.wait()
    for i in range(nb):
        for cp in xload(i):
            cp.wait()
        activations(x[i], dy[i], w, dab)
        if i == 0:
            dwa_in.wait()
        else:
            dxr_in.wait()
            dxr_out.start()
            dw0_in.wait()
            dw0_out.start()
            gp_in.wait()
            gy_in.wait()
            for c in range(NCH):
                gn[c // 2, :, (c % 2) * CW:(c % 2 + 1) * CW] = gp[c].astype(F32) + gy[c].astype(F32)
        dxs[i] = (dxa[i] + input_grad(w, dab)).astype(BF)
        for k in range(3):
            weight_grad(k, x[i], dy[i], dab, dw, False)
            if i == nb - 1:
                dw_out(k).start()
        dx_out(i).start()
        if i == nb - 1:
            gn_out.start()
    for i in range(nb):
        dx_out(i).wait()
    for k in range(3):
        dw_out(k).wait()
    for cp in (dxr_out, dw0_out, gn_out):
        cp.wait()


def fused_step(x, dy, w1, w3, w2, g):
    any_space = pl.BlockSpec(memory_space=pl.ANY)
    dma = pltpu.SemaphoreType.DMA
    vmem = pltpu.VMEM
    sds = jax.ShapeDtypeStruct
    nb = NBLK - NB1
    scratch = [
        vmem((T, D), BF), vmem((T, D), BF), vmem((2, 3, HQ, D), BF),
        vmem((T, D), F32), vmem((2, TB, D), BF), vmem((3, TB, HQ), BF), vmem((3, 2, HS, D), F32),
        vmem((3, 4, HS, CW), F32), vmem((NCH, 2, 2, HS, CW), BF), vmem((NCH, 2, HS, CW), BF), vmem((NCH, HS, CW), BF),
        dma((NBLK,)), dma((NBLK,)), dma((3,)), dma((3,)), dma((2,)), dma, dma, dma((3,)), dma, dma((NCH,)),
        dma((3,)), dma((3,)), dma((NWP,)), dma((NWP,)), dma((NWP,)), dma((NWP,)), dma((2, NWP)), dma((2, NWP)),
        dma((NCH,)), dma((NCH,)), dma((NCH,)), dma((NCH,)), dma((NCH,)), dma((NCH,)),
    ]
    part = sds((3, 2, HS, D), F32)
    chunks = sds((NCH, HS, CW), BF)
    carried = pl.pallas_call(
        first_kernel,
        out_shape=(sds((NB1 * TB, D), BF), sds((nb * TB, D), F32), part, part, sds((3, HQ, D), BF), chunks, chunks),
        in_specs=[any_space] * 6,
        out_specs=(any_space,) * 7,
        scratch_shapes=scratch,
        compiler_params=pltpu.CompilerParams(collective_id=0, has_side_effects=True, vmem_limit_bytes=67043328),
    )(x, dy, w1, w3, w2, g)
    scratch = [
        vmem((nb, TB, D), BF), vmem((nb, TB, D), BF), vmem((3, HQ, D), BF), vmem((NB1 * TB, D), BF), vmem((nb, TB, D), F32),
        vmem((nb, TB, D), BF), vmem((3, TB, HQ), BF), vmem((3, 2, HS, D), F32), vmem((3, 2, HS, D), F32),
        vmem((NCH, HS, CW), BF), vmem((NCH, HS, CW), BF), vmem((3, HS, D), F32),
        dma((nb,)), dma((nb,)), dma, dma((nb,)), dma((5,)), dma((nb,)), dma((3,)), dma((3,)),
    ]
    return pl.pallas_call(
        second_kernel,
        out_shape=(sds((T, D), BF), sds((3, 4, HS, D), F32), sds((3, HS, D), F32)),
        in_specs=[any_space] * 9,
        out_specs=(any_space,) * 3,
        scratch_shapes=scratch,
        compiler_params=pltpu.CompilerParams(vmem_limit_bytes=67043328),
    )(x, dy, *carried)


def solution(mesh):
    def per_device(x_blk, dy_blk, gate_shard, up_shard, down_shard, g_part):
        g_t = jnp.swapaxes(g_part[0], 1, 2).reshape(3, 4, HS, D)
        dx_blk, dwt, gnt = fused_step(x_blk, dy_blk, gate_shard.T, up_shard.T, down_shard, g_t)
        dw_local = jnp.swapaxes(dwt.reshape(3, H, D), 1, 2)
        return dx_blk, jnp.swapaxes(gnt, 1, 2), dw_local[None]

    return jax.shard_map(
        per_device,
        mesh=mesh,
        in_specs=(P(ALL_AXES, None), P(ALL_AXES, None), P(None, GROUP_AXES), P(None, GROUP_AXES), P(GROUP_AXES, None), P(ALL_AXES, None, None, None)),
        out_specs=(P(ALL_AXES, None), P(None, None, GROUP_AXES), P(ALL_AXES, None, None, None)),
        check_vma=False,
    )
```

```python
import functools

import jax
import jax.numpy as jnp
from jax import lax
from jax.experimental import pallas as pl
from jax.experimental.pallas import tpu as pltpu
from jax.sharding import PartitionSpec as P

GROUP_AXES = ("row", "fsdp")
ALL_AXES = ("dp", "row", "fsdp")
MESH = pl.DeviceIdType.MESH
BF, F32 = jnp.bfloat16, jnp.float32

T, D, H = 4096, 512, 1376
HS = H // 4
HSP = 384
HQ = 2 * HSP
TB = 1024
NBLK = T // TB
NCH, CW = 6, 256
NWP, WW = 6, 128
NT_COLS, GATE_ROWS = 256, 64
NB1 = 2

NN = (((1,), (0,)), ((), ()))
NT = (((1,), (1,)), ((), ()))
TN = (((0,), (0,)), ((), ()))


def dot(a, b, dims):
    return lax.dot_general(a, b, dims, preferred_element_type=F32)


def gate_grads(a, b, dh):
    sig = 0.5 * jnp.tanh(0.5 * a) + 0.5
    silu = a * sig
    h = (silu * b).astype(BF)
    da = (dh * b * sig * (1.0 + a * (1.0 - sig))).astype(BF)
    db = (dh * silu).astype(BF)
    return h, da, db


def block_rows(i):
    return pl.ds(i * TB if isinstance(i, int) else pl.multiple_of(i * TB, TB), TB)


def activations(xb, dyb, w, dab):
    for c in range(0, HQ, NT_COLS):
        cols = slice(c, c + NT_COLS)
        a = dot(xb, w[0, cols], NT)
        b = dot(xb, w[1, cols], NT)
        dh = dot(dyb, w[2, cols], NT)
        for r in range(0, TB, GATE_ROWS):
            rows = slice(r, r + GATE_ROWS)
            h, da, db = gate_grads(a[rows], b[rows], dh[rows])
            dab[0, rows, cols], dab[1, rows, cols], dab[2, rows, cols] = da, db, h


def input_grad(w, dab):
    return dot(dab[0], w[0], NN) + dot(dab[1], w[1], NN)


def weight_grad(k, xb, dyb, dab, dw, fresh):
    for s in range(2):
        part = dot(dab[k, :, s * HSP:s * HSP + HS], dyb if k == 2 else xb, TN)
        if fresh is True:
            dw[k, s] = part
        elif fresh is False:
            dw[k, s] = dw[k, s] + part
        else:
            dw[k, s] = jnp.where(fresh, 0.0, dw[k, s]) + part


def first_kernel(x_hbm, dy_hbm, w1_hbm, w3_hbm, w2_hbm, g_hbm,
                 dxr_hbm, dxa_hbm, dw0_hbm, dwa_hbm, w_hbm, gp_hbm, gy_hbm,
                 x, dy, wall, dxa, dxs, dab, dw, gst, pk, prec, xrec,
                 x_sem, dy_sem, ws_sem, g_sem, dx_sem, dxa_sem, dw0_sem, dwa_sem, w_sem, gp_sem,
                 a1s, a1r, a2s, a2r, a3s, a3r, a4s, a4r, ps, pr, xs_, xr_, ys_, yr_):
    dp, row, f = (lax.axis_index(n) for n in ALL_AXES)
    partner, xn, yn = {"fsdp": 1 - f}, {"row": 1 - row}, {"dp": 1 - dp}
    mine = pl.ds(pl.multiple_of(f * HSP, HSP), HS)

    def xload(i):
        rows = block_rows(i)
        return (pltpu.make_async_copy(x_hbm.at[rows], x.at[rows], x_sem.at[i]),
                pltpu.make_async_copy(dy_hbm.at[rows], dy.at[rows], dy_sem.at[i]))

    def gload(c):
        return pltpu.make_async_copy(g_hbm.at[c // 2, :, :, pl.ds((c % 2) * CW, CW)], gst.at[c % 3], g_sem.at[c % 3])

    def remote(src, dst, s, r, dev):
        return pltpu.make_async_remote_copy(src_ref=src, dst_ref=dst, send_sem=s, recv_sem=r, device_id=dev, device_id_type=MESH)

    def wload(m):
        return pltpu.make_async_copy((w1_hbm, w3_hbm, w2_hbm)[m], wall.at[0, m, mine], ws_sem.at[m])

    def a1(m):
        ref = wall.at[0, m, mine]
        return remote(ref, ref, a1s.at[m], a1r.at[m], partner)

    def piece(p, j, half):
        return wall.at[p, j // 2, mine, pl.ds(pl.multiple_of(half * 256 + (j % 2) * WW, WW), WW)]

    def a2(j):
        return remote(piece(0, j, dp), piece(1, j, dp), a2s.at[j], a2r.at[j], xn)

    def a3(j):
        ref = piece(1, j, dp)
        return remote(ref, ref, a3s.at[j], a3r.at[j], yn)

    def a4(n, j, half):
        ref = piece(1, j, half)
        return remote(ref, ref, a4s.at[n, j], a4r.at[n, j], partner)

    def psend(c):
        return remote(pk.at[c, 1 - f], prec.at[c], ps.at[c], pr.at[c], partner)

    def xsend(c):
        return remote(pk.at[c, f, 1 - row], xrec.at[c], xs_.at[c], xr_.at[c], xn)

    def ysend(c):
        return remote(pk.at[c, f, row], gy_hbm.at[c], ys_.at[c], yr_.at[c], yn)

    def gp_out(c):
        return pltpu.make_async_copy(pk.at[c, f, row], gp_hbm.at[c], gp_sem.at[c])

    def dx_out(i):
        return pltpu.make_async_copy(dxs.at[i % 2], dxr_hbm.at[block_rows(i)], dx_sem.at[i % 2])

    def dwa_out(k):
        return pltpu.make_async_copy(dw.at[k], dwa_hbm.at[k], dwa_sem.at[k])

    dw0_out = pltpu.make_async_copy(dw, dw0_hbm, dw0_sem)
    dxa_out = pltpu.make_async_copy(dxa.at[pl.ds(NB1 * TB, T - NB1 * TB)], dxa_hbm, dxa_sem)
    w_out = pltpu.make_async_copy(wall.at[1], w_hbm, w_sem)

    def convert(c):
        gload(c).wait()
        for s in range(4):
            pk[c, s % 2, s // 2] = gst[c % 3, s].astype(BF)

    edge = HS // 16 * 16
    for p in range(2):
        for m in range(3):
            for k in range(2):
                wall[p, m, k * HSP + edge:(k + 1) * HSP, :] = jnp.zeros((HSP - edge, D), BF)
    for m in range(3):
        wload(m).start()
    for c in range(2):
        gload(c).start()
    for cp in xload(0):
        cp.start()
    gload(2).start()
    barrier = pltpu.get_barrier_semaphore()
    for dev in (partner, xn, yn):
        pl.semaphore_signal(barrier, inc=1, device_id=dev, device_id_type=MESH)
    pl.semaphore_wait(barrier, 3)
    for m in range(3):
        wload(m).wait()
        a1(m).start()
        a2(2 * m).start()
        a2(2 * m + 1).start()
    for c in range(2):
        convert(c)
        gload(c + 3).start()
    for i in range(1, NBLK):
        for cp in xload(i):
            cp.start()
    for c in range(2):
        psend(c).start()
    for m in range(3):
        a1(m).wait_recv()

    def add1(c):
        psend(c).wait_recv()
        for k in range(2):
            pk[c, f, k] = (pk[c, f, k].astype(F32) + prec[c, k].astype(F32)).astype(BF)

    def add2(c):
        xsend(c).wait_recv()
        pk[c, f, row] = (pk[c, f, row].astype(F32) + xrec[c].astype(F32)).astype(BF)

    def w_first(j):
        a2(j).wait_recv()
        a3(j).start()
        a4(0, j, dp).start()

    def w_second(j):
        a3(j).wait_recv()
        a4(1, j, 1 - dp).start()

    plan = {
        2: ((0, 1, 2, 3), (), (2, 3, 4), (0, 1), ()),
        4: ((4, 5), (), (5,), (2, 3, 4), (0,)),
        6: ((), (0, 1, 2, 3, 4, 5), (), (5,), (1, 2)),
        8: ((), (), (), (), (3, 4)),
        9: ((), (), (), (), (5,)),
    }

    def actions(n):
        first, second, conv, chip, over_x = plan[n]
        for j in first:
            w_first(j)
        for j in second:
            w_second(j)
        for c in conv:
            convert(c)
            if c + 3 < NCH:
                gload(c + 3).start()
        for c in chip:
            add1(c)
        for c in over_x:
            add2(c)
        for c in conv:
            psend(c).start()
        for c in chip:
            xsend(c).start()
        for c in over_x:
            ysend(c).start()
            gp_out(c).start()

    def body(i, carry):
        rows = block_rows(i)
        for cp in xload(i):
            cp.wait()
        for blk in range(NBLK):
            if 2 * blk in plan:
                pl.when(i == blk)(functools.partial(actions, 2 * blk))
        activations(x[rows, :], dy[rows, :], wall.at[0], dab)
        dxa[rows, :] = input_grad(wall.at[0], dab)
        for k in range(3):
            weight_grad(k, x[rows, :], dy[rows, :], dab, dw, i == 0)
        return carry

    lax.fori_loop(0, NBLK, body, 0)
    dw0_out.start()
    dxa_out.start()
    for j in range(NWP):
        a4(0, j, dp).wait_recv()
        a4(1, j, 1 - dp).wait_recv()
    w_out.start()

    for i in range(NB1):
        rows = block_rows(i)
        n = 2 * (NBLK + i)
        if n in plan:
            actions(n)
        activations(x[rows, :], dy[rows, :], wall.at[1], dab)
        if n + 1 in plan:
            actions(n + 1)
        if i == 0:
            dw0_out.wait()
        for k in range(3):
            weight_grad(k, x[rows, :], dy[rows, :], dab, dw, i == 0)
            if i == NB1 - 1:
                dwa_out(k).start()
        dxs[i % 2] = (dxa[rows, :] + input_grad(wall.at[1], dab)).astype(BF)
        dx_out(i).start()

    for m in range(3):
        a1(m).wait_send()
    for j in range(NWP):
        a2(j).wait_send()
        a3(j).wait_send()
        a4(0, j, dp).wait_send()
        a4(1, j, 1 - dp).wait_send()
    for c in range(NCH):
        psend(c).wait_send()
        xsend(c).wait_send()
        ysend(c).wait_send()
        gp_out(c).wait()
    for i in range(NB1):
        dx_out(i).wait()
    dxa_out.wait()
    w_out.wait()
    for k in range(3):
        dwa_out(k).wait()
    for c in range(NCH):
        ysend(c).wait_recv()


def second_kernel(x_hbm, dy_hbm, dxr_hbm, dxa_hbm, dw0_hbm, dwa_hbm, w_hbm, gp_hbm, gy_hbm,
                  dx_hbm, dwt_hbm, gn_hbm,
                  x, dy, w, dxr, dxa, dxs, dab, dw, dw0, gp, gy, gn,
                  x_sem, dy_sem, w_sem, dxa_sem, in_sem, dx_sem, dw_sem, out_sem):
    row = lax.axis_index("row")
    nb = NBLK - NB1

    def xload(i):
        rows = block_rows(NB1 + i)
        return (pltpu.make_async_copy(x_hbm.at[rows], x.at[i], x_sem.at[i]),
                pltpu.make_async_copy(dy_hbm.at[rows], dy.at[i], dy_sem.at[i]),
                pltpu.make_async_copy(dxa_hbm.at[block_rows(i)], dxa.at[i], dxa_sem.at[i]))

    def dx_out(i):
        return pltpu.make_async_copy(dxs.at[i], dx_hbm.at[block_rows(NB1 + i)], dx_sem.at[i])

    def dw_out(k):
        return pltpu.make_async_copy(dw.at[k], dwt_hbm.at[k, pl.ds(2 * (1 - row), 2)], dw_sem.at[k])

    w_in = pltpu.make_async_copy(w_hbm, w, w_sem)
    dwa_in, gp_in, gy_in, dxr_in, dw0_in = (
        pltpu.make_async_copy(src, dst, in_sem.at[n])
        for n, (src, dst) in enumerate([(dwa_hbm, dw), (gp_hbm, gp), (gy_hbm, gy), (dxr_hbm, dxr), (dw0_hbm, dw0)]))
    dxr_out = pltpu.make_async_copy(dxr, dx_hbm.at[pl.ds(0, NB1 * TB)], out_sem.at[0])
    dw0_out = pltpu.make_async_copy(dw0, dwt_hbm.at[:, pl.ds(2 * row, 2)], out_sem.at[1])
    gn_out = pltpu.make_async_copy(gn, gn_hbm, out_sem.at[2])

    w_in.start()
    for cp in xload(0)[:2]:
        cp.start()
    dwa_in.start()
    xload(0)[2].start()
    for i in range(1, nb):
        for cp in xload(i):
            cp.start()
    for cp in (gp_in, gy_in, dxr_in, dw0_in):
        cp.start()
    w_in.wait()
    for i in range(nb):
        x_in, dy_in, dxa_in = xload(i)
        x_in.wait()
        dy_in.wait()
        activations(x[i], dy[i], w, dab)
        if i == 0:
            dwa_in.wait()
        for k in range(3):
            weight_grad(k, x[i], dy[i], dab, dw, False)
            if i == nb - 1:
                dw_out(k).start()
        dxa_in.wait()
        dxs[i] = (dxa[i] + input_grad(w, dab)).astype(BF)
        dx_out(i).start()
        if i == 0:
            dxr_in.wait()
            dxr_out.start()
            dw0_in.wait()
            dw0_out.start()
            gp_in.wait()
            gy_in.wait()
            for c in range(NCH):
                gn[c // 2, :, (c % 2) * CW:(c % 2 + 1) * CW] = gp[c].astype(F32) + gy[c].astype(F32)
            gn_out.start()
    for i in range(nb):
        dx_out(i).wait()
    for k in range(3):
        dw_out(k).wait()
    for cp in (dxr_out, dw0_out, gn_out):
        cp.wait()


def fused_step(x, dy, w1, w3, w2, g):
    any_space = pl.BlockSpec(memory_space=pl.ANY)
    dma = pltpu.SemaphoreType.DMA
    vmem = pltpu.VMEM
    sds = jax.ShapeDtypeStruct
    nb = NBLK - NB1
    scratch = [
        vmem((T, D), BF), vmem((T, D), BF), vmem((2, 3, HQ, D), BF),
        vmem((T, D), F32), vmem((2, TB, D), BF), vmem((3, TB, HQ), BF), vmem((3, 2, HS, D), F32),
        vmem((3, 4, HS, CW), F32), vmem((NCH, 2, 2, HS, CW), BF), vmem((NCH, 2, HS, CW), BF), vmem((NCH, HS, CW), BF),
        dma((NBLK,)), dma((NBLK,)), dma((3,)), dma((3,)), dma((2,)), dma, dma, dma((3,)), dma, dma((NCH,)),
        dma((3,)), dma((3,)), dma((NWP,)), dma((NWP,)), dma((NWP,)), dma((NWP,)), dma((2, NWP)), dma((2, NWP)),
        dma((NCH,)), dma((NCH,)), dma((NCH,)), dma((NCH,)), dma((NCH,)), dma((NCH,)),
    ]
    part = sds((3, 2, HS, D), F32)
    chunks = sds((NCH, HS, CW), BF)
    carried = pl.pallas_call(
        first_kernel,
        out_shape=(sds((NB1 * TB, D), BF), sds((nb * TB, D), F32), part, part, sds((3, HQ, D), BF), chunks, chunks),
        in_specs=[any_space] * 6,
        out_specs=(any_space,) * 7,
        scratch_shapes=scratch,
        compiler_params=pltpu.CompilerParams(collective_id=0, has_side_effects=True, vmem_limit_bytes=67043328),
    )(x, dy, w1, w3, w2, g)
    scratch = [
        vmem((nb, TB, D), BF), vmem((nb, TB, D), BF), vmem((3, HQ, D), BF), vmem((NB1 * TB, D), BF), vmem((nb, TB, D), F32),
        vmem((nb, TB, D), BF), vmem((3, TB, HQ), BF), vmem((3, 2, HS, D), F32), vmem((3, 2, HS, D), F32),
        vmem((NCH, HS, CW), BF), vmem((NCH, HS, CW), BF), vmem((3, HS, D), F32),
        dma((nb,)), dma((nb,)), dma, dma((nb,)), dma((5,)), dma((nb,)), dma((3,)), dma((3,)),
    ]
    return pl.pallas_call(
        second_kernel,
        out_shape=(sds((T, D), BF), sds((3, 4, HS, D), F32), sds((3, HS, D), F32)),
        in_specs=[any_space] * 9,
        out_specs=(any_space,) * 3,
        scratch_shapes=scratch,
        compiler_params=pltpu.CompilerParams(vmem_limit_bytes=67043328),
    )(x, dy, *carried)


def solution(mesh):
    def per_device(x_blk, dy_blk, gate_shard, up_shard, down_shard, g_part):
        g_t = jnp.swapaxes(g_part[0], 1, 2).reshape(3, 4, HS, D)
        dx_blk, dwt, gnt = fused_step(x_blk, dy_blk, gate_shard.T, up_shard.T, down_shard, g_t)
        dw_local = jnp.swapaxes(dwt.reshape(3, H, D), 1, 2)
        return dx_blk, jnp.swapaxes(gnt, 1, 2), dw_local[None]

    return jax.shard_map(
        per_device,
        mesh=mesh,
        in_specs=(P(ALL_AXES, None), P(ALL_AXES, None), P(None, GROUP_AXES), P(None, GROUP_AXES), P(GROUP_AXES, None), P(ALL_AXES, None, None, None)),
        out_specs=(P(ALL_AXES, None), P(None, None, GROUP_AXES), P(ALL_AXES, None, None, None)),
        check_vma=False,
    )
```

```python
import functools

import jax
import jax.numpy as jnp
from jax import lax
from jax.experimental import pallas as pl
from jax.experimental.pallas import tpu as pltpu
from jax.sharding import PartitionSpec as P

GROUP_AXES = ("row", "fsdp")
ALL_AXES = ("dp", "row", "fsdp")
MESH = pl.DeviceIdType.MESH
BF, F32 = jnp.bfloat16, jnp.float32

T, D, H = 4096, 512, 1376
HS = H // 4
HSP = 384
HQ = 2 * HSP
TB = 1024
NBLK = T // TB
NCH, CW = 6, 256
NWP, WW = 6, 128
NT_COLS, GATE_ROWS = 256, 64
NB1 = 2

NN = (((1,), (0,)), ((), ()))
NT = (((1,), (1,)), ((), ()))
TN = (((0,), (0,)), ((), ()))


def dot(a, b, dims):
    return lax.dot_general(a, b, dims, preferred_element_type=F32)


def gate_grads(a, b, dh):
    sig = 0.5 * jnp.tanh(0.5 * a) + 0.5
    silu = a * sig
    h = (silu * b).astype(BF)
    da = (dh * b * sig * (1.0 + a * (1.0 - sig))).astype(BF)
    db = (dh * silu).astype(BF)
    return h, da, db


def block_rows(i):
    return pl.ds(i * TB if isinstance(i, int) else pl.multiple_of(i * TB, TB), TB)


def activations(xb, dyb, w, dab, before=lambda tile: None):
    for c in range(0, HQ, NT_COLS):
        before(c // NT_COLS)
        cols = slice(c, c + NT_COLS)
        a = dot(xb, w[0, cols], NT)
        b = dot(xb, w[1, cols], NT)
        dh = dot(dyb, w[2, cols], NT)
        for r in range(0, TB, GATE_ROWS):
            rows = slice(r, r + GATE_ROWS)
            h, da, db = gate_grads(a[rows], b[rows], dh[rows])
            dab[0, rows, cols], dab[1, rows, cols], dab[2, rows, cols] = da, db, h


def input_grad(w, dab):
    return dot(dab[0], w[0], NN) + dot(dab[1], w[1], NN)


def weight_grad(k, xb, dyb, dab, dw, fresh):
    for s in range(2):
        part = dot(dab[k, :, s * HSP:s * HSP + HS], dyb if k == 2 else xb, TN)
        if fresh is True:
            dw[k, s] = part
        elif fresh is False:
            dw[k, s] = dw[k, s] + part
        else:
            dw[k, s] = jnp.where(fresh, 0.0, dw[k, s]) + part


def first_kernel(x_hbm, dy_hbm, w1_hbm, w3_hbm, w2_hbm, g_hbm,
                 dxr_hbm, dxa_hbm, dw0_hbm, dwa_hbm, w_hbm, gp_hbm, gy_hbm,
                 x, dy, wall, dxa, dxs, dab, dw, gst, pk, prec, xrec,
                 x_sem, dy_sem, ws_sem, g_sem, dx_sem, dxa_sem, dw0_sem, dwa_sem, w_sem, gp_sem,
                 a1s, a1r, a2s, a2r, a3s, a3r, a4s, a4r, ps, pr, xs_, xr_, ys_, yr_):
    dp, row, f = (lax.axis_index(n) for n in ALL_AXES)
    partner, xn, yn = {"fsdp": 1 - f}, {"row": 1 - row}, {"dp": 1 - dp}
    mine = pl.ds(pl.multiple_of(f * HSP, HSP), HS)

    def xload(i):
        rows = block_rows(i)
        return (pltpu.make_async_copy(x_hbm.at[rows], x.at[rows], x_sem.at[i]),
                pltpu.make_async_copy(dy_hbm.at[rows], dy.at[rows], dy_sem.at[i]))

    def gload(c):
        return pltpu.make_async_copy(g_hbm.at[c // 2, :, :, pl.ds((c % 2) * CW, CW)], gst.at[c % 3], g_sem.at[c % 3])

    def remote(src, dst, s, r, dev):
        return pltpu.make_async_remote_copy(src_ref=src, dst_ref=dst, send_sem=s, recv_sem=r, device_id=dev, device_id_type=MESH)

    def wload(m):
        return pltpu.make_async_copy((w1_hbm, w3_hbm, w2_hbm)[m], wall.at[0, m, mine], ws_sem.at[m])

    def a1(m):
        ref = wall.at[0, m, mine]
        return remote(ref, ref, a1s.at[m], a1r.at[m], partner)

    def piece(p, j, half):
        return wall.at[p, j // 2, mine, pl.ds(pl.multiple_of(half * 256 + (j % 2) * WW, WW), WW)]

    def a2(j):
        return remote(piece(0, j, dp), piece(1, j, dp), a2s.at[j], a2r.at[j], xn)

    def a3(j):
        ref = piece(1, j, dp)
        return remote(ref, ref, a3s.at[j], a3r.at[j], yn)

    def a4(n, j, half):
        ref = piece(1, j, half)
        return remote(ref, ref, a4s.at[n, j], a4r.at[n, j], partner)

    def psend(c):
        return remote(pk.at[c, 1 - f], prec.at[c], ps.at[c], pr.at[c], partner)

    def xsend(c):
        return remote(pk.at[c, f, 1 - row], xrec.at[c], xs_.at[c], xr_.at[c], xn)

    def ysend(c):
        return remote(pk.at[c, f, row], gy_hbm.at[c], ys_.at[c], yr_.at[c], yn)

    def gp_out(c):
        return pltpu.make_async_copy(pk.at[c, f, row], gp_hbm.at[c], gp_sem.at[c])

    def dx_out(i):
        return pltpu.make_async_copy(dxs.at[i % 2], dxr_hbm.at[block_rows(i)], dx_sem.at[i % 2])

    def dwa_out(k):
        return pltpu.make_async_copy(dw.at[k], dwa_hbm.at[k], dwa_sem.at[k])

    dw0_out = pltpu.make_async_copy(dw, dw0_hbm, dw0_sem)
    dxa_out = pltpu.make_async_copy(dxa.at[pl.ds(NB1 * TB, T - NB1 * TB)], dxa_hbm, dxa_sem)
    w_out = pltpu.make_async_copy(wall.at[1], w_hbm, w_sem)

    def convert(c):
        gload(c).wait()
        for s in range(4):
            pk[c, s % 2, s // 2] = gst[c % 3, s].astype(BF)

    edge = HS // 16 * 16
    for p in range(2):
        for m in range(3):
            for k in range(2):
                wall[p, m, k * HSP + edge:(k + 1) * HSP, :] = jnp.zeros((HSP - edge, D), BF)
    for m in range(3):
        wload(m).start()
    barrier = pltpu.get_barrier_semaphore()
    for dev in (partner, xn, yn):
        pl.semaphore_signal(barrier, inc=1, device_id=dev, device_id_type=MESH)
    pl.semaphore_wait(barrier, 3)
    for m in range(3):
        wload(m).wait()
        a1(m).start()
        a2(2 * m).start()
        a2(2 * m + 1).start()
    for cp in xload(0):
        cp.start()
    for c in range(2):
        gload(c).start()
    for c in range(2):
        convert(c)
    for c in range(2):
        psend(c).start()
    for m in range(3):
        a1(m).wait_recv()
    for c in range(2, 5):
        gload(c).start()
    for i in range(1, NBLK):
        for cp in xload(i):
            cp.start()

    def add1(c):
        psend(c).wait_recv()
        for k in range(2):
            pk[c, f, k] = (pk[c, f, k].astype(F32) + prec[c, k].astype(F32)).astype(BF)

    def add2(c):
        xsend(c).wait_recv()
        pk[c, f, row] = (pk[c, f, row].astype(F32) + xrec[c].astype(F32)).astype(BF)

    def w_first(j):
        a2(j).wait_recv()
        a3(j).start()
        a4(0, j, dp).start()

    def w_second(j):
        a3(j).wait_recv()
        a4(1, j, 1 - dp).start()

    plan = {
        2: ((0, 1, 2, 3), (), (2, 3, 4), (0, 1), ()),
        4: ((4, 5), (), (5,), (2, 3, 4), (0,)),
        6: ((), (0, 1, 2, 3, 4, 5), (), (5,), (1, 2)),
        8: ((), (), (), (), (3, 4)),
        9: ((), (), (), (), (5,)),
    }

    def actions(n):
        first, second, conv, chip, over_x = plan[n]
        for j in first:
            w_first(j)
        for j in second:
            w_second(j)
        for c in conv:
            convert(c)
            if 5 <= c + 3 < NCH:
                gload(c + 3).start()
        for c in chip:
            add1(c)
        for c in over_x:
            add2(c)
        for c in conv:
            psend(c).start()
        for c in chip:
            xsend(c).start()
        for c in over_x:
            ysend(c).start()
            gp_out(c).start()

    def body(i, carry):
        rows = block_rows(i)
        for cp in xload(i):
            cp.wait()
        for blk in range(NBLK):
            if 2 * blk in plan:
                pl.when(i == blk)(functools.partial(actions, 2 * blk))
        activations(x[rows, :], dy[rows, :], wall.at[0], dab)
        dxa[rows, :] = input_grad(wall.at[0], dab)
        for k in range(3):
            weight_grad(k, x[rows, :], dy[rows, :], dab, dw, i == 0)
        return carry

    lax.fori_loop(0, NBLK, body, 0)
    dw0_out.start()
    dxa_out.start()
    for j in range(NWP):
        a4(0, j, dp).wait_recv()
        a4(1, j, 1 - dp).wait_recv()
    w_out.start()

    for i in range(NB1):
        rows = block_rows(i)
        n = 2 * (NBLK + i)
        if n in plan:
            actions(n)
        activations(x[rows, :], dy[rows, :], wall.at[1], dab)
        if n + 1 in plan:
            actions(n + 1)
        if i == 0:
            dw0_out.wait()
        for k in range(3):
            weight_grad(k, x[rows, :], dy[rows, :], dab, dw, i == 0)
            if i == NB1 - 1:
                dwa_out(k).start()
        dxs[i % 2] = (dxa[rows, :] + input_grad(wall.at[1], dab)).astype(BF)
        dx_out(i).start()

    for m in range(3):
        a1(m).wait_send()
    for j in range(NWP):
        a2(j).wait_send()
        a3(j).wait_send()
        a4(0, j, dp).wait_send()
        a4(1, j, 1 - dp).wait_send()
    for c in range(NCH):
        psend(c).wait_send()
        xsend(c).wait_send()
        ysend(c).wait_send()
        gp_out(c).wait()
    for i in range(NB1):
        dx_out(i).wait()
    dxa_out.wait()
    w_out.wait()
    for k in range(3):
        dwa_out(k).wait()
    for c in range(NCH):
        ysend(c).wait_recv()


def second_kernel(x_hbm, dy_hbm, dxr_hbm, dxa_hbm, dw0_hbm, dwa_hbm, w_hbm, gp_hbm, gy_hbm,
                  dx_hbm, dwt_hbm, gn_hbm,
                  x, dy, w, dxr, dxa, dxs, dab, dw, dw0, gp, gy, gn,
                  x_sem, dy_sem, w_sem, dxa_sem, in_sem, dx_sem, dw_sem, out_sem):
    row = lax.axis_index("row")
    nb = NBLK - NB1

    def xload(i):
        rows = block_rows(NB1 + i)
        return (pltpu.make_async_copy(x_hbm.at[rows], x.at[i], x_sem.at[i]),
                pltpu.make_async_copy(dy_hbm.at[rows], dy.at[i], dy_sem.at[i]),
                pltpu.make_async_copy(dxa_hbm.at[block_rows(i)], dxa.at[i], dxa_sem.at[i]))

    def dx_out(i):
        return pltpu.make_async_copy(dxs.at[i], dx_hbm.at[block_rows(NB1 + i)], dx_sem.at[i])

    def dw_out(k):
        return pltpu.make_async_copy(dw.at[k], dwt_hbm.at[k, pl.ds(2 * (1 - row), 2)], dw_sem.at[k])

    def w_in(t):
        rows = pl.ds(t * NT_COLS, NT_COLS)
        return pltpu.make_async_copy(w_hbm.at[:, rows], w.at[:, rows], w_sem.at[t])

    dwa_in, gp_in, gy_in, dxr_in, dw0_in = (
        pltpu.make_async_copy(src, dst, in_sem.at[n])
        for n, (src, dst) in enumerate([(dwa_hbm, dw), (gp_hbm, gp), (gy_hbm, gy), (dxr_hbm, dxr), (dw0_hbm, dw0)]))
    dxr_out = pltpu.make_async_copy(dxr, dx_hbm.at[pl.ds(0, NB1 * TB)], out_sem.at[0])
    dw0_out = pltpu.make_async_copy(dw0, dwt_hbm.at[:, pl.ds(2 * row, 2)], out_sem.at[1])
    gn_out = pltpu.make_async_copy(gn, gn_hbm, out_sem.at[2])

    tiles = HQ // NT_COLS
    x_in, dy_in, dxa_in = zip(*[xload(i) for i in range(nb)])
    w_in(0).start()
    x_in[0].start()
    dy_in[0].start()
    for t in range(1, tiles):
        w_in(t).start()
    x_in[0].wait()
    dy_in[0].wait()
    for i in range(nb):
        last = i == nb - 1
        if i > 0:
            x_in[i].wait()
            dy_in[i].wait()

        def before(t):
            if i == 0:
                w_in(t).wait()
                if t == tiles - 1:
                    dwa_in.start()
                    dxa_in[0].start()

        activations(x[i], dy[i], w, dab, before)
        if i == 0:
            dwa_in.wait()
        if not last:
            for cp in (x_in[i + 1], dy_in[i + 1], dxa_in[i + 1]):
                cp.start()
        if i == 0:
            dxr_in.start()
            dw0_in.start()
        if last:
            gp_in.wait()
            gy_in.wait()
            for c in range(NCH):
                gn[c // 2, :, (c % 2) * CW:(c % 2 + 1) * CW] = gp[c].astype(F32) + gy[c].astype(F32)
            gn_out.start()
        for k in range(3):
            weight_grad(k, x[i], dy[i], dab, dw, False)
            if last:
                dw_out(k).start()
        dxa_in[i].wait()
        if i == 0:
            gp_in.start()
            gy_in.start()
        dxs[i] = (dxa[i] + input_grad(w, dab)).astype(BF)
        dx_out(i).start()
        if i == 0:
            dxr_in.wait()
            dxr_out.start()
            dw0_in.wait()
            dw0_out.start()
    for i in range(nb):
        dx_out(i).wait()
    for k in range(3):
        dw_out(k).wait()
    for cp in (dxr_out, dw0_out, gn_out):
        cp.wait()


def fused_step(x, dy, w1, w3, w2, g):
    any_space = pl.BlockSpec(memory_space=pl.ANY)
    dma = pltpu.SemaphoreType.DMA
    vmem = pltpu.VMEM
    sds = jax.ShapeDtypeStruct
    nb = NBLK - NB1
    scratch = [
        vmem((T, D), BF), vmem((T, D), BF), vmem((2, 3, HQ, D), BF),
        vmem((T, D), F32), vmem((2, TB, D), BF), vmem((3, TB, HQ), BF), vmem((3, 2, HS, D), F32),
        vmem((3, 4, HS, CW), F32), vmem((NCH, 2, 2, HS, CW), BF), vmem((NCH, 2, HS, CW), BF), vmem((NCH, HS, CW), BF),
        dma((NBLK,)), dma((NBLK,)), dma((3,)), dma((3,)), dma((2,)), dma, dma, dma((3,)), dma, dma((NCH,)),
        dma((3,)), dma((3,)), dma((NWP,)), dma((NWP,)), dma((NWP,)), dma((NWP,)), dma((2, NWP)), dma((2, NWP)),
        dma((NCH,)), dma((NCH,)), dma((NCH,)), dma((NCH,)), dma((NCH,)), dma((NCH,)),
    ]
    part = sds((3, 2, HS, D), F32)
    chunks = sds((NCH, HS, CW), BF)
    carried = pl.pallas_call(
        first_kernel,
        out_shape=(sds((NB1 * TB, D), BF), sds((nb * TB, D), F32), part, part, sds((3, HQ, D), BF), chunks, chunks),
        in_specs=[any_space] * 6,
        out_specs=(any_space,) * 7,
        scratch_shapes=scratch,
        compiler_params=pltpu.CompilerParams(collective_id=0, has_side_effects=True, vmem_limit_bytes=67043328),
    )(x, dy, w1, w3, w2, g)
    scratch = [
        vmem((nb, TB, D), BF), vmem((nb, TB, D), BF), vmem((3, HQ, D), BF), vmem((NB1 * TB, D), BF), vmem((nb, TB, D), F32),
        vmem((nb, TB, D), BF), vmem((3, TB, HQ), BF), vmem((3, 2, HS, D), F32), vmem((3, 2, HS, D), F32),
        vmem((NCH, HS, CW), BF), vmem((NCH, HS, CW), BF), vmem((3, HS, D), F32),
        dma((nb,)), dma((nb,)), dma((HQ // NT_COLS,)), dma((nb,)), dma((5,)), dma((nb,)), dma((3,)), dma((3,)),
    ]
    return pl.pallas_call(
        second_kernel,
        out_shape=(sds((T, D), BF), sds((3, 4, HS, D), F32), sds((3, HS, D), F32)),
        in_specs=[any_space] * 9,
        out_specs=(any_space,) * 3,
        scratch_shapes=scratch,
        compiler_params=pltpu.CompilerParams(vmem_limit_bytes=67043328),
    )(x, dy, *carried)


def solution(mesh):
    def per_device(x_blk, dy_blk, gate_shard, up_shard, down_shard, g_part):
        g_t = jnp.swapaxes(g_part[0], 1, 2).reshape(3, 4, HS, D)
        dx_blk, dwt, gnt = fused_step(x_blk, dy_blk, gate_shard.T, up_shard.T, down_shard, g_t)
        dw_local = jnp.swapaxes(dwt.reshape(3, H, D), 1, 2)
        return dx_blk, jnp.swapaxes(gnt, 1, 2), dw_local[None]

    return jax.shard_map(
        per_device,
        mesh=mesh,
        in_specs=(P(ALL_AXES, None), P(ALL_AXES, None), P(None, GROUP_AXES), P(None, GROUP_AXES), P(GROUP_AXES, None), P(ALL_AXES, None, None, None)),
        out_specs=(P(ALL_AXES, None), P(None, None, GROUP_AXES), P(ALL_AXES, None, None, None)),
        check_vma=False,
    )
```

```python
import functools

import jax
import jax.numpy as jnp
from jax import lax
from jax.experimental import pallas as pl
from jax.experimental.pallas import tpu as pltpu
from jax.sharding import PartitionSpec as P

GROUP_AXES = ("row", "fsdp")
ALL_AXES = ("dp", "row", "fsdp")
MESH = pl.DeviceIdType.MESH
BF, F32 = jnp.bfloat16, jnp.float32

T, D, H = 4096, 512, 1376
HS = H // 4
HSP = 384
HQ = 2 * HSP
TB = 1024
NBLK = T // TB
NCH, CW = 6, 256
NWP, WW = 6, 128
NT_COLS, GATE_ROWS = 256, 64
NB1 = 2

NN = (((1,), (0,)), ((), ()))
NT = (((1,), (1,)), ((), ()))
TN = (((0,), (0,)), ((), ()))


def dot(a, b, dims):
    return lax.dot_general(a, b, dims, preferred_element_type=F32)


def gate_grads(a, b, dh):
    sig = 0.5 * jnp.tanh(0.5 * a) + 0.5
    silu = a * sig
    h = (silu * b).astype(BF)
    da = (dh * b * sig * (1.0 + a * (1.0 - sig))).astype(BF)
    db = (dh * silu).astype(BF)
    return h, da, db


def block_rows(i):
    return pl.ds(i * TB if isinstance(i, int) else pl.multiple_of(i * TB, TB), TB)


def activations(xb, dyb, w, dab, before=lambda tile: None):
    for c in range(0, HQ, NT_COLS):
        before(c // NT_COLS)
        cols = slice(c, c + NT_COLS)
        a = dot(xb, w[0, cols], NT)
        b = dot(xb, w[1, cols], NT)
        dh = dot(dyb, w[2, cols], NT)
        for r in range(0, TB, GATE_ROWS):
            rows = slice(r, r + GATE_ROWS)
            h, da, db = gate_grads(a[rows], b[rows], dh[rows])
            dab[0, rows, cols], dab[1, rows, cols], dab[2, rows, cols] = da, db, h


def input_grad(w, dab):
    return dot(dab[0], w[0], NN) + dot(dab[1], w[1], NN)


def weight_grad(k, xb, dyb, dab, dw, fresh):
    for s in range(2):
        part = dot(dab[k, :, s * HSP:s * HSP + HS], dyb if k == 2 else xb, TN)
        if fresh is True:
            dw[k, s] = part
        elif fresh is False:
            dw[k, s] = dw[k, s] + part
        else:
            dw[k, s] = jnp.where(fresh, 0.0, dw[k, s]) + part


def first_kernel(x_hbm, dy_hbm, w1_hbm, w3_hbm, w2_hbm, g_hbm,
                 dxr_hbm, dxa_hbm, dw0_hbm, dwa_hbm, w_hbm, gp_hbm, gy_hbm,
                 x, dy, wall, dxa, dxs, dab, dw, gst, pk, prec, xrec,
                 x_sem, dy_sem, ws_sem, g_sem, dx_sem, dxa_sem, dw0_sem, dwa_sem, w_sem, gp_sem,
                 a1s, a1r, a2s, a2r, a3s, a3r, a4s, a4r, ps, pr, xs_, xr_, ys_, yr_):
    dp, row, f = (lax.axis_index(n) for n in ALL_AXES)
    partner, xn, yn = {"fsdp": 1 - f}, {"row": 1 - row}, {"dp": 1 - dp}
    mine = pl.ds(pl.multiple_of(f * HSP, HSP), HS)

    def xload(i):
        rows = block_rows(i)
        return (pltpu.make_async_copy(x_hbm.at[rows], x.at[rows], x_sem.at[i]),
                pltpu.make_async_copy(dy_hbm.at[rows], dy.at[rows], dy_sem.at[i]))

    def gload(c):
        return pltpu.make_async_copy(g_hbm.at[c // 2, :, :, pl.ds((c % 2) * CW, CW)], gst.at[c % 3], g_sem.at[c % 3])

    def remote(src, dst, s, r, dev):
        return pltpu.make_async_remote_copy(src_ref=src, dst_ref=dst, send_sem=s, recv_sem=r, device_id=dev, device_id_type=MESH)

    def wload(m):
        return pltpu.make_async_copy((w1_hbm, w3_hbm, w2_hbm)[m], wall.at[0, m, mine], ws_sem.at[m])

    def a1(m):
        ref = wall.at[0, m, mine]
        return remote(ref, ref, a1s.at[m], a1r.at[m], partner)

    def piece(p, j, half):
        return wall.at[p, j // 2, mine, pl.ds(pl.multiple_of(half * 256 + (j % 2) * WW, WW), WW)]

    def a2(j):
        return remote(piece(0, j, dp), piece(1, j, dp), a2s.at[j], a2r.at[j], xn)

    def a3(j):
        ref = piece(1, j, dp)
        return remote(ref, ref, a3s.at[j], a3r.at[j], yn)

    def a4(n, j, half):
        ref = piece(1, j, half)
        return remote(ref, ref, a4s.at[n, j], a4r.at[n, j], partner)

    def psend(c):
        return remote(pk.at[c, 1 - f], prec.at[c], ps.at[c], pr.at[c], partner)

    def xsend(c):
        return remote(pk.at[c, f, 1 - row], xrec.at[c], xs_.at[c], xr_.at[c], xn)

    def ysend(c):
        return remote(pk.at[c, f, row], gy_hbm.at[c], ys_.at[c], yr_.at[c], yn)

    def gp_out(c):
        return pltpu.make_async_copy(pk.at[c, f, row], gp_hbm.at[c], gp_sem.at[c])

    def dx_out(i):
        return pltpu.make_async_copy(dxs.at[i % 2], dxr_hbm.at[block_rows(i)], dx_sem.at[i % 2])

    def dwa_out(k):
        return pltpu.make_async_copy(dw.at[k], dwa_hbm.at[k], dwa_sem.at[k])

    dw0_out = pltpu.make_async_copy(dw, dw0_hbm, dw0_sem)
    dxa_out = pltpu.make_async_copy(dxa.at[pl.ds(NB1 * TB, T - NB1 * TB)], dxa_hbm, dxa_sem)
    w_out = pltpu.make_async_copy(wall.at[1], w_hbm, w_sem)

    def convert(c):
        gload(c).wait()
        for s in range(4):
            pk[c, s % 2, s // 2] = gst[c % 3, s].astype(BF)

    edge = HS // 16 * 16
    for p in range(2):
        for m in range(3):
            for k in range(2):
                wall[p, m, k * HSP + edge:(k + 1) * HSP, :] = jnp.zeros((HSP - edge, D), BF)
    for m in range(3):
        wload(m).start()
    barrier = pltpu.get_barrier_semaphore()
    for dev in (partner, xn, yn):
        pl.semaphore_signal(barrier, inc=1, device_id=dev, device_id_type=MESH)
    pl.semaphore_wait(barrier, 3)
    for m in range(3):
        wload(m).wait()
        a1(m).start()
    for j in range(NWP):
        a2(j).start()
    for cp in xload(0):
        cp.start()
    for c in range(2):
        gload(c).start()
    for c in range(2):
        convert(c)
    for m in range(3):
        a1(m).wait_recv()
    for c in range(2):
        psend(c).start()
    for c in range(2, 5):
        gload(c).start()
    for i in range(1, NBLK):
        for cp in xload(i):
            cp.start()

    def add1(c):
        psend(c).wait_recv()
        for k in range(2):
            pk[c, f, k] = (pk[c, f, k].astype(F32) + prec[c, k].astype(F32)).astype(BF)

    def add2(c):
        xsend(c).wait_recv()
        pk[c, f, row] = (pk[c, f, row].astype(F32) + xrec[c].astype(F32)).astype(BF)

    def w_first(j):
        a2(j).wait_recv()
        a3(j).start()
        a4(0, j, dp).start()

    def w_second(j):
        a3(j).wait_recv()
        a4(1, j, 1 - dp).start()

    plan = {
        2: ((0, 1, 2, 3), (), (2, 3, 4), (0, 1), ()),
        4: ((4, 5), (), (5,), (2, 3, 4), (0,)),
        6: ((), (0, 1, 2, 3, 4, 5), (), (5,), (1, 2)),
        8: ((), (), (), (), (3, 4)),
        9: ((), (), (), (), (5,)),
    }

    def actions(n):
        first, second, conv, chip, over_x = plan[n]
        for j in first:
            w_first(j)
        for j in second:
            w_second(j)
        for c in conv:
            convert(c)
            if 5 <= c + 3 < NCH:
                gload(c + 3).start()
        for c in chip:
            add1(c)
        for c in over_x:
            add2(c)
        for c in conv:
            psend(c).start()
        for c in chip:
            xsend(c).start()
        for c in over_x:
            ysend(c).start()
            gp_out(c).start()

    def body(i, carry):
        rows = block_rows(i)
        for cp in xload(i):
            cp.wait()
        for blk in range(NBLK):
            if 2 * blk in plan:
                pl.when(i == blk)(functools.partial(actions, 2 * blk))
        activations(x[rows, :], dy[rows, :], wall.at[0], dab)
        dxa[rows, :] = input_grad(wall.at[0], dab)
        for k in range(3):
            weight_grad(k, x[rows, :], dy[rows, :], dab, dw, i == 0)
        return carry

    lax.fori_loop(0, NBLK, body, 0)
    dw0_out.start()
    for j in range(NWP):
        a4(0, j, dp).wait_recv()
        a4(1, j, 1 - dp).wait_recv()

    for i in range(NB1):
        rows = block_rows(i)
        n = 2 * (NBLK + i)
        if n in plan:
            actions(n)
        activations(x[rows, :], dy[rows, :], wall.at[1], dab)
        if n + 1 in plan:
            actions(n + 1)
        if i == 0:
            dw0_out.wait()
            dxa_out.start()
            w_out.start()
        for k in range(3):
            weight_grad(k, x[rows, :], dy[rows, :], dab, dw, i == 0)
            if i == NB1 - 1:
                dwa_out(k).start()
        dxs[i % 2] = (dxa[rows, :] + input_grad(wall.at[1], dab)).astype(BF)
        dx_out(i).start()

    for m in range(3):
        a1(m).wait_send()
    for j in range(NWP):
        a2(j).wait_send()
        a3(j).wait_send()
        a4(0, j, dp).wait_send()
        a4(1, j, 1 - dp).wait_send()
    for c in range(NCH):
        psend(c).wait_send()
        xsend(c).wait_send()
        ysend(c).wait_send()
        gp_out(c).wait()
    for i in range(NB1):
        dx_out(i).wait()
    dxa_out.wait()
    w_out.wait()
    for k in range(3):
        dwa_out(k).wait()
    for c in range(NCH):
        ysend(c).wait_recv()


def second_kernel(x_hbm, dy_hbm, dxr_hbm, dxa_hbm, dw0_hbm, dwa_hbm, w_hbm, gp_hbm, gy_hbm,
                  dx_hbm, dwt_hbm, gn_hbm,
                  x, dy, w, dxr, dxa, dxs, dab, dw, dw0, gp, gy, gn,
                  x_sem, dy_sem, w_sem, dxa_sem, in_sem, dx_sem, dw_sem, out_sem):
    row = lax.axis_index("row")
    nb = NBLK - NB1

    def xload(i):
        rows = block_rows(NB1 + i)
        return (pltpu.make_async_copy(x_hbm.at[rows], x.at[i], x_sem.at[i]),
                pltpu.make_async_copy(dy_hbm.at[rows], dy.at[i], dy_sem.at[i]),
                pltpu.make_async_copy(dxa_hbm.at[block_rows(i)], dxa.at[i], dxa_sem.at[i]))

    def dx_out(i):
        return pltpu.make_async_copy(dxs.at[i], dx_hbm.at[block_rows(NB1 + i)], dx_sem.at[i])

    def dw_out(k):
        return pltpu.make_async_copy(dw.at[k], dwt_hbm.at[k, pl.ds(2 * (1 - row), 2)], dw_sem.at[k])

    def w_in(t):
        rows = pl.ds(t * NT_COLS, NT_COLS)
        return pltpu.make_async_copy(w_hbm.at[:, rows], w.at[:, rows], w_sem.at[t])

    dwa_in, gp_in, gy_in, dxr_in, dw0_in = (
        pltpu.make_async_copy(src, dst, in_sem.at[n])
        for n, (src, dst) in enumerate([(dwa_hbm, dw), (gp_hbm, gp), (gy_hbm, gy), (dxr_hbm, dxr), (dw0_hbm, dw0)]))
    dxr_out = pltpu.make_async_copy(dxr, dx_hbm.at[pl.ds(0, NB1 * TB)], out_sem.at[0])
    dw0_out = pltpu.make_async_copy(dw0, dwt_hbm.at[:, pl.ds(2 * row, 2)], out_sem.at[1])
    gn_out = pltpu.make_async_copy(gn, gn_hbm, out_sem.at[2])

    tiles = HQ // NT_COLS
    x_in, dy_in, dxa_in = zip(*[xload(i) for i in range(nb)])
    w_in(0).start()
    x_in[0].start()
    dy_in[0].start()
    x_in[0].wait()
    dy_in[0].wait()
    for i in range(nb):
        first, last = i == 0, i == nb - 1
        if not first:
            x_in[i].wait()
            dy_in[i].wait()

        def before(t):
            if first:
                w_in(t).wait()
                if t == 0:
                    for n in range(1, tiles):
                        w_in(n).start()
                if t == 1:
                    dxa_in[0].start()
                    dwa_in.start()
            elif last and t == tiles - 1:
                dxr_in.wait()
                dxr_out.start()
                dw0_in.wait()
                dw0_out.start()

        activations(x[i], dy[i], w, dab, before)
        if not last:
            for cp in (x_in[i + 1], dy_in[i + 1], dxa_in[i + 1]):
                cp.start()
        if last:
            gp_in.wait()
            gy_in.wait()
            for c in range(NCH):
                gn[c // 2, :, (c % 2) * CW:(c % 2 + 1) * CW] = gp[c].astype(F32) + gy[c].astype(F32)
            gn_out.start()
            for k in range(3):
                weight_grad(k, x[i], dy[i], dab, dw, False)
                dw_out(k).start()
        dxa_in[i].wait()
        dxs[i] = (dxa[i] + input_grad(w, dab)).astype(BF)
        dx_out(i).start()
        if first:
            for cp in (dxr_in, dw0_in, gp_in, gy_in):
                cp.start()
            dwa_in.wait()
        if not last:
            for k in range(3):
                weight_grad(k, x[i], dy[i], dab, dw, False)
    for i in range(nb):
        dx_out(i).wait()
    for k in range(3):
        dw_out(k).wait()
    for cp in (dxr_out, dw0_out, gn_out):
        cp.wait()


def fused_step(x, dy, w1, w3, w2, g):
    any_space = pl.BlockSpec(memory_space=pl.ANY)
    dma = pltpu.SemaphoreType.DMA
    vmem = pltpu.VMEM
    sds = jax.ShapeDtypeStruct
    nb = NBLK - NB1
    scratch = [
        vmem((T, D), BF), vmem((T, D), BF), vmem((2, 3, HQ, D), BF),
        vmem((T, D), F32), vmem((2, TB, D), BF), vmem((3, TB, HQ), BF), vmem((3, 2, HS, D), F32),
        vmem((3, 4, HS, CW), F32), vmem((NCH, 2, 2, HS, CW), BF), vmem((NCH, 2, HS, CW), BF), vmem((NCH, HS, CW), BF),
        dma((NBLK,)), dma((NBLK,)), dma((3,)), dma((3,)), dma((2,)), dma, dma, dma((3,)), dma, dma((NCH,)),
        dma((3,)), dma((3,)), dma((NWP,)), dma((NWP,)), dma((NWP,)), dma((NWP,)), dma((2, NWP)), dma((2, NWP)),
        dma((NCH,)), dma((NCH,)), dma((NCH,)), dma((NCH,)), dma((NCH,)), dma((NCH,)),
    ]
    part = sds((3, 2, HS, D), F32)
    chunks = sds((NCH, HS, CW), BF)
    carried = pl.pallas_call(
        first_kernel,
        out_shape=(sds((NB1 * TB, D), BF), sds((nb * TB, D), F32), part, part, sds((3, HQ, D), BF), chunks, chunks),
        in_specs=[any_space] * 6,
        out_specs=(any_space,) * 7,
        scratch_shapes=scratch,
        compiler_params=pltpu.CompilerParams(collective_id=0, has_side_effects=True, vmem_limit_bytes=67043328),
    )(x, dy, w1, w3, w2, g)
    scratch = [
        vmem((nb, TB, D), BF), vmem((nb, TB, D), BF), vmem((3, HQ, D), BF), vmem((NB1 * TB, D), BF), vmem((nb, TB, D), F32),
        vmem((nb, TB, D), BF), vmem((3, TB, HQ), BF), vmem((3, 2, HS, D), F32), vmem((3, 2, HS, D), F32),
        vmem((NCH, HS, CW), BF), vmem((NCH, HS, CW), BF), vmem((3, HS, D), F32),
        dma((nb,)), dma((nb,)), dma((HQ // NT_COLS,)), dma((nb,)), dma((5,)), dma((nb,)), dma((3,)), dma((3,)),
    ]
    return pl.pallas_call(
        second_kernel,
        out_shape=(sds((T, D), BF), sds((3, 4, HS, D), F32), sds((3, HS, D), F32)),
        in_specs=[any_space] * 9,
        out_specs=(any_space,) * 3,
        scratch_shapes=scratch,
        compiler_params=pltpu.CompilerParams(vmem_limit_bytes=67043328),
    )(x, dy, *carried)


def solution(mesh):
    def per_device(x_blk, dy_blk, gate_shard, up_shard, down_shard, g_part):
        g_t = jnp.swapaxes(g_part[0], 1, 2).reshape(3, 4, HS, D)
        dx_blk, dwt, gnt = fused_step(x_blk, dy_blk, gate_shard.T, up_shard.T, down_shard, g_t)
        dw_local = jnp.swapaxes(dwt.reshape(3, H, D), 1, 2)
        return dx_blk, jnp.swapaxes(gnt, 1, 2), dw_local[None]

    return jax.shard_map(
        per_device,
        mesh=mesh,
        in_specs=(P(ALL_AXES, None), P(ALL_AXES, None), P(None, GROUP_AXES), P(None, GROUP_AXES), P(GROUP_AXES, None), P(ALL_AXES, None, None, None)),
        out_specs=(P(ALL_AXES, None), P(None, None, GROUP_AXES), P(ALL_AXES, None, None, None)),
        check_vma=False,
    )
```

```python
import functools

import jax
import jax.numpy as jnp
from jax import lax
from jax.experimental import pallas as pl
from jax.experimental.pallas import tpu as pltpu
from jax.sharding import PartitionSpec as P

GROUP_AXES = ("row", "fsdp")
ALL_AXES = ("dp", "row", "fsdp")
MESH = pl.DeviceIdType.MESH
BF, F32 = jnp.bfloat16, jnp.float32

T, D, H = 4096, 512, 1376
HS = H // 4
HSP = 384
HQ = 2 * HSP
TB = 1024
NBLK = T // TB
NCH, CW = 6, 256
NWP, WW = 6, 128
NT_COLS, GATE_ROWS = 256, 64
HB = TB // 2
NB1 = 2

NN = (((1,), (0,)), ((), ()))
NT = (((1,), (1,)), ((), ()))
TN = (((0,), (0,)), ((), ()))


def dot(a, b, dims):
    return lax.dot_general(a, b, dims, preferred_element_type=F32)


def gate_grads(a, b, dh):
    sig = 0.5 * jnp.tanh(0.5 * a) + 0.5
    silu = a * sig
    h = (silu * b).astype(BF)
    da = (dh * b * sig * (1.0 + a * (1.0 - sig))).astype(BF)
    db = (dh * silu).astype(BF)
    return h, da, db


def block_rows(i):
    return pl.ds(i * TB if isinstance(i, int) else pl.multiple_of(i * TB, TB), TB)


def activations(xb, dyb, w, dab, before=lambda tile: None):
    for c in range(0, HQ, NT_COLS):
        before(c // NT_COLS)
        cols = slice(c, c + NT_COLS)
        a = dot(xb, w[0, cols], NT)
        b = dot(xb, w[1, cols], NT)
        dh = dot(dyb, w[2, cols], NT)
        for r in range(0, TB, GATE_ROWS):
            rows = slice(r, r + GATE_ROWS)
            h, da, db = gate_grads(a[rows], b[rows], dh[rows])
            dab[0, rows, cols], dab[1, rows, cols], dab[2, rows, cols] = da, db, h


def input_grad(w, dab, rows=slice(0, TB)):
    return dot(dab[0, rows], w[0], NN) + dot(dab[1, rows], w[1], NN)


def weight_grad(k, xb, dyb, dab, dw, fresh):
    for s in range(2):
        part = dot(dab[k, :, s * HSP:s * HSP + HS], dyb if k == 2 else xb, TN)
        if fresh is True:
            dw[k, s] = part
        elif fresh is False:
            dw[k, s] = dw[k, s] + part
        else:
            dw[k, s] = jnp.where(fresh, 0.0, dw[k, s]) + part


def first_kernel(x_hbm, dy_hbm, w1_hbm, w3_hbm, w2_hbm, g_hbm,
                 dxr_hbm, dxa_hbm, dw0_hbm, dwa_hbm, w_hbm, gp_hbm, gy_hbm,
                 x, dy, wall, dxa, dxs, dab, dw, gst, pk, prec, xrec,
                 x_sem, dy_sem, ws_sem, g_sem, dx_sem, dxa_sem, dw0_sem, dwa_sem, w_sem, gp_sem,
                 a1s, a1r, a2s, a2r, a3s, a3r, a4s, a4r, ps, pr, xs_, xr_, ys_, yr_):
    dp, row, f = (lax.axis_index(n) for n in ALL_AXES)
    partner, xn, yn = {"fsdp": 1 - f}, {"row": 1 - row}, {"dp": 1 - dp}
    mine = pl.ds(pl.multiple_of(f * HSP, HSP), HS)

    def xload(i):
        rows = block_rows(i)
        return (pltpu.make_async_copy(x_hbm.at[rows], x.at[rows], x_sem.at[i]),
                pltpu.make_async_copy(dy_hbm.at[rows], dy.at[rows], dy_sem.at[i]))

    def gload(c):
        return pltpu.make_async_copy(g_hbm.at[c // 2, :, :, pl.ds((c % 2) * CW, CW)], gst.at[c % 3], g_sem.at[c % 3])

    def remote(src, dst, s, r, dev):
        return pltpu.make_async_remote_copy(src_ref=src, dst_ref=dst, send_sem=s, recv_sem=r, device_id=dev, device_id_type=MESH)

    def wload(m):
        return pltpu.make_async_copy((w1_hbm, w3_hbm, w2_hbm)[m], wall.at[0, m, mine], ws_sem.at[m])

    def a1(m):
        ref = wall.at[0, m, mine]
        return remote(ref, ref, a1s.at[m], a1r.at[m], partner)

    def piece(p, j, half):
        return wall.at[p, j // 2, mine, pl.ds(pl.multiple_of(half * 256 + (j % 2) * WW, WW), WW)]

    def a2(j):
        return remote(piece(0, j, dp), piece(1, j, dp), a2s.at[j], a2r.at[j], xn)

    def a3(j):
        ref = piece(1, j, dp)
        return remote(ref, ref, a3s.at[j], a3r.at[j], yn)

    def a4(n, j, half):
        ref = piece(1, j, half)
        return remote(ref, ref, a4s.at[n, j], a4r.at[n, j], partner)

    def psend(c):
        return remote(pk.at[c, 1 - f], prec.at[c], ps.at[c], pr.at[c], partner)

    def xsend(c):
        return remote(pk.at[c, f, 1 - row], xrec.at[c], xs_.at[c], xr_.at[c], xn)

    def ysend(c):
        return remote(pk.at[c, f, row], gy_hbm.at[c], ys_.at[c], yr_.at[c], yn)

    def gp_out(c):
        return pltpu.make_async_copy(pk.at[c, f, row], gp_hbm.at[c], gp_sem.at[c])

    def dx_out(i):
        return [pltpu.make_async_copy(dxs.at[i, pl.ds(h, HB)], dxr_hbm.at[pl.ds(i * TB + h, HB)], dx_sem.at[i, h // HB]) for h in (0, HB)]

    def dwa_out(k):
        return pltpu.make_async_copy(dw.at[k], dwa_hbm.at[k], dwa_sem.at[k])

    dw0_out = pltpu.make_async_copy(dw, dw0_hbm, dw0_sem)
    dxa_out = pltpu.make_async_copy(dxa.at[pl.ds(NB1 * TB, T - NB1 * TB)], dxa_hbm, dxa_sem)
    w_out = pltpu.make_async_copy(wall.at[1], w_hbm, w_sem)

    def convert(c):
        gload(c).wait()
        for s in range(4):
            pk[c, s % 2, s // 2] = gst[c % 3, s].astype(BF)

    edge = HS // 16 * 16
    for p in range(2):
        for m in range(3):
            for k in range(2):
                wall[p, m, k * HSP + edge:(k + 1) * HSP, :] = jnp.zeros((HSP - edge, D), BF)
    for m in range(3):
        wload(m).start()
    barrier = pltpu.get_barrier_semaphore()
    for dev in (partner, xn, yn):
        pl.semaphore_signal(barrier, inc=1, device_id=dev, device_id_type=MESH)
    pl.semaphore_wait(barrier, 3)
    for m in range(3):
        wload(m).wait()
        a1(m).start()
    for j in range(NWP):
        a2(j).start()
    for cp in xload(0):
        cp.start()
    for c in range(2):
        gload(c).start()
    for c in range(2):
        convert(c)
    for m in range(3):
        a1(m).wait_recv()
    for c in range(2):
        psend(c).start()
    for c in range(2, 5):
        gload(c).start()
    for i in range(1, NBLK):
        for cp in xload(i):
            cp.start()

    def add1(c):
        psend(c).wait_recv()
        for k in range(2):
            pk[c, f, k] = (pk[c, f, k].astype(F32) + prec[c, k].astype(F32)).astype(BF)

    def add2(c):
        xsend(c).wait_recv()
        pk[c, f, row] = (pk[c, f, row].astype(F32) + xrec[c].astype(F32)).astype(BF)

    def w_first(j):
        a2(j).wait_recv()
        a3(j).start()
        a4(0, j, dp).start()

    def w_second(j):
        a3(j).wait_recv()
        a4(1, j, 1 - dp).start()

    plan = {
        2: ((0, 1, 2, 3), (), (2, 3, 4), (0, 1), ()),
        4: ((4, 5), (), (5,), (2, 3, 4), (0,)),
        6: ((), (0, 1, 2, 3, 4, 5), (), (5,), (1, 2)),
        8: ((), (), (), (), (3, 4)),
        9: ((), (), (), (), (5,)),
    }

    def actions(n):
        first, second, conv, chip, over_x = plan[n]
        for j in first:
            w_first(j)
        for j in second:
            w_second(j)
        for c in conv:
            convert(c)
            if 5 <= c + 3 < NCH:
                gload(c + 3).start()
        for c in chip:
            add1(c)
        for c in over_x:
            add2(c)
        for c in conv:
            psend(c).start()
        for c in chip:
            xsend(c).start()
        for c in over_x:
            ysend(c).start()
            gp_out(c).start()

    def body(i, carry):
        rows = block_rows(i)
        for cp in xload(i):
            cp.wait()
        for blk in range(NBLK):
            if 2 * blk in plan:
                pl.when(i == blk)(functools.partial(actions, 2 * blk))
        activations(x[rows, :], dy[rows, :], wall.at[0], dab)
        dxa[rows, :] = input_grad(wall.at[0], dab)
        for k in range(3):
            weight_grad(k, x[rows, :], dy[rows, :], dab, dw, i == 0)
        return carry

    lax.fori_loop(0, NBLK, body, 0)
    dw0_out.start()
    for j in range(NWP):
        a4(0, j, dp).wait_recv()
        a4(1, j, 1 - dp).wait_recv()

    for i in range(NB1):
        rows = block_rows(i)
        n = 2 * (NBLK + i)
        if n in plan:
            actions(n)
        activations(x[rows, :], dy[rows, :], wall.at[1], dab)
        if n + 1 in plan:
            actions(n + 1)
        if i == 0:
            dw0_out.wait()
            dxa_out.start()
            w_out.start()
        for k in range(3):
            weight_grad(k, x[rows, :], dy[rows, :], dab, dw, i == 0)
            if i == NB1 - 1:
                dwa_out(k).start()
        for h, cp in zip((0, HB), dx_out(i)):
            part = slice(h, h + HB)
            dxs[i, part] = (dxa[i * TB + h:i * TB + h + HB, :] + input_grad(wall.at[1], dab, part)).astype(BF)
            cp.start()

    for m in range(3):
        a1(m).wait_send()
    for j in range(NWP):
        a2(j).wait_send()
        a3(j).wait_send()
        a4(0, j, dp).wait_send()
        a4(1, j, 1 - dp).wait_send()
    for c in range(NCH):
        psend(c).wait_send()
        xsend(c).wait_send()
        ysend(c).wait_send()
        gp_out(c).wait()
    for i in range(NB1):
        for cp in dx_out(i):
            cp.wait()
    dxa_out.wait()
    w_out.wait()
    for k in range(3):
        dwa_out(k).wait()
    for c in range(NCH):
        ysend(c).wait_recv()


def second_kernel(x_hbm, dy_hbm, dxr_hbm, dxa_hbm, dw0_hbm, dwa_hbm, w_hbm, gp_hbm, gy_hbm,
                  dx_hbm, dwt_hbm, gn_hbm,
                  x, dy, w, dxr, dxa, dxs, dab, dw, dw0, gp, gy, gn,
                  x_sem, dy_sem, w_sem, dxa_sem, in_sem, dx_sem, dw_sem, out_sem):
    row = lax.axis_index("row")
    nb = NBLK - NB1

    def xload(i):
        rows = block_rows(NB1 + i)
        return (pltpu.make_async_copy(x_hbm.at[rows], x.at[i], x_sem.at[i]),
                pltpu.make_async_copy(dy_hbm.at[rows], dy.at[i], dy_sem.at[i]),
                pltpu.make_async_copy(dxa_hbm.at[block_rows(i)], dxa.at[i], dxa_sem.at[i]))

    def dx_out(i):
        return [pltpu.make_async_copy(dxs.at[i, pl.ds(h, HB)], dx_hbm.at[pl.ds((NB1 + i) * TB + h, HB)], dx_sem.at[i, h // HB]) for h in (0, HB)]

    def dw_out(k):
        return pltpu.make_async_copy(dw.at[k], dwt_hbm.at[k, pl.ds(2 * (1 - row), 2)], dw_sem.at[k])

    def w_in(t):
        rows = pl.ds(t * NT_COLS, NT_COLS)
        return pltpu.make_async_copy(w_hbm.at[:, rows], w.at[:, rows], w_sem.at[t])

    dwa_in, gp_in, gy_in, dxr_in, dw0_in = (
        pltpu.make_async_copy(src, dst, in_sem.at[n])
        for n, (src, dst) in enumerate([(dwa_hbm, dw), (gp_hbm, gp), (gy_hbm, gy), (dxr_hbm, dxr), (dw0_hbm, dw0)]))
    dxr_out = pltpu.make_async_copy(dxr, dx_hbm.at[pl.ds(0, NB1 * TB)], out_sem.at[0])
    dw0_out = pltpu.make_async_copy(dw0, dwt_hbm.at[:, pl.ds(2 * row, 2)], out_sem.at[1])
    gn_out = pltpu.make_async_copy(gn, gn_hbm, out_sem.at[2])

    tiles = HQ // NT_COLS
    x_in, dy_in, dxa_in = zip(*[xload(i) for i in range(nb)])
    w_in(0).start()
    x_in[0].start()
    dy_in[0].start()
    x_in[0].wait()
    dy_in[0].wait()
    for i in range(nb):
        first, last = i == 0, i == nb - 1
        if not first:
            x_in[i].wait()
            dy_in[i].wait()

        def before(t):
            if first:
                w_in(t).wait()
                if t == 0:
                    for n in range(1, tiles):
                        w_in(n).start()
                if t == 1:
                    dxa_in[0].start()
                    dwa_in.start()
            elif last and t == tiles - 1:
                dxr_in.wait()
                dxr_out.start()
                dw0_in.wait()
                dw0_out.start()

        activations(x[i], dy[i], w, dab, before)
        if not last:
            for cp in (x_in[i + 1], dy_in[i + 1], dxa_in[i + 1]):
                cp.start()
        if last:
            gp_in.wait()
            gy_in.wait()
            for c in range(NCH):
                gn[c // 2, :, (c % 2) * CW:(c % 2 + 1) * CW] = gp[c].astype(F32) + gy[c].astype(F32)
            gn_out.start()
            for k in range(3):
                weight_grad(k, x[i], dy[i], dab, dw, False)
                dw_out(k).start()
        dxa_in[i].wait()
        for h, cp in zip((0, HB), dx_out(i)):
            part = slice(h, h + HB)
            dxs[i, part] = (dxa[i, part] + input_grad(w, dab, part)).astype(BF)
            cp.start()
        if first:
            for cp in (dxr_in, dw0_in, gp_in, gy_in):
                cp.start()
            dwa_in.wait()
        if not last:
            for k in range(3):
                weight_grad(k, x[i], dy[i], dab, dw, False)
    for i in range(nb):
        for cp in dx_out(i):
            cp.wait()
    for k in range(3):
        dw_out(k).wait()
    for cp in (dxr_out, dw0_out, gn_out):
        cp.wait()


def fused_step(x, dy, w1, w3, w2, g):
    any_space = pl.BlockSpec(memory_space=pl.ANY)
    dma = pltpu.SemaphoreType.DMA
    vmem = pltpu.VMEM
    sds = jax.ShapeDtypeStruct
    nb = NBLK - NB1
    scratch = [
        vmem((T, D), BF), vmem((T, D), BF), vmem((2, 3, HQ, D), BF),
        vmem((T, D), F32), vmem((NB1, TB, D), BF), vmem((3, TB, HQ), BF), vmem((3, 2, HS, D), F32),
        vmem((3, 4, HS, CW), F32), vmem((NCH, 2, 2, HS, CW), BF), vmem((NCH, 2, HS, CW), BF), vmem((NCH, HS, CW), BF),
        dma((NBLK,)), dma((NBLK,)), dma((3,)), dma((3,)), dma((NB1, 2)), dma, dma, dma((3,)), dma, dma((NCH,)),
        dma((3,)), dma((3,)), dma((NWP,)), dma((NWP,)), dma((NWP,)), dma((NWP,)), dma((2, NWP)), dma((2, NWP)),
        dma((NCH,)), dma((NCH,)), dma((NCH,)), dma((NCH,)), dma((NCH,)), dma((NCH,)),
    ]
    part = sds((3, 2, HS, D), F32)
    chunks = sds((NCH, HS, CW), BF)
    carried = pl.pallas_call(
        first_kernel,
        out_shape=(sds((NB1 * TB, D), BF), sds((nb * TB, D), F32), part, part, sds((3, HQ, D), BF), chunks, chunks),
        in_specs=[any_space] * 6,
        out_specs=(any_space,) * 7,
        scratch_shapes=scratch,
        compiler_params=pltpu.CompilerParams(collective_id=0, has_side_effects=True, vmem_limit_bytes=67043328),
    )(x, dy, w1, w3, w2, g)
    scratch = [
        vmem((nb, TB, D), BF), vmem((nb, TB, D), BF), vmem((3, HQ, D), BF), vmem((NB1 * TB, D), BF), vmem((nb, TB, D), F32),
        vmem((nb, TB, D), BF), vmem((3, TB, HQ), BF), vmem((3, 2, HS, D), F32), vmem((3, 2, HS, D), F32),
        vmem((NCH, HS, CW), BF), vmem((NCH, HS, CW), BF), vmem((3, HS, D), F32),
        dma((nb,)), dma((nb,)), dma((HQ // NT_COLS,)), dma((nb,)), dma((5,)), dma((nb, 2)), dma((3,)), dma((3,)),
    ]
    return pl.pallas_call(
        second_kernel,
        out_shape=(sds((T, D), BF), sds((3, 4, HS, D), F32), sds((3, HS, D), F32)),
        in_specs=[any_space] * 9,
        out_specs=(any_space,) * 3,
        scratch_shapes=scratch,
        compiler_params=pltpu.CompilerParams(vmem_limit_bytes=67043328),
    )(x, dy, *carried)


def solution(mesh):
    def per_device(x_blk, dy_blk, gate_shard, up_shard, down_shard, g_part):
        g_t = jnp.swapaxes(g_part[0], 1, 2).reshape(3, 4, HS, D)
        dx_blk, dwt, gnt = fused_step(x_blk, dy_blk, gate_shard.T, up_shard.T, down_shard, g_t)
        dw_local = jnp.swapaxes(dwt.reshape(3, H, D), 1, 2)
        return dx_blk, jnp.swapaxes(gnt, 1, 2), dw_local[None]

    return jax.shard_map(
        per_device,
        mesh=mesh,
        in_specs=(P(ALL_AXES, None), P(ALL_AXES, None), P(None, GROUP_AXES), P(None, GROUP_AXES), P(GROUP_AXES, None), P(ALL_AXES, None, None, None)),
        out_specs=(P(ALL_AXES, None), P(None, None, GROUP_AXES), P(ALL_AXES, None, None, None)),
        check_vma=False,
    )
```
